32 devices in a mesh: groups: 2 (over x), kv: 16 (over z, y, core).
Axes of the slice: x: 2, y: 2, z: 4, core: 2. Of those that a mesh axis runs over, the one named last changes fastest.
Arguments:
- queries: bfloat16 [80, 18432], P('groups', 'kv'), parts along dimension 0, may hold values from -240 to 240
- latent_cache: bfloat16 [80, 2048, 576], P('groups', 'kv'), parts along dimension 0, may hold values from -6 to 6
- context_lengths: int32 [80], P('groups'), parts along dimension 0, may hold values from 128 to 2048, as said below
- value_up: bfloat16 [16384, 128], P('kv'), may hold values from -0.25 to 0.25
- out_proj: bfloat16 [4096, 7168], P('kv'), may hold values from -0.09375 to 0.09375
- residual: bfloat16 [80, 7168], P('groups', 'kv'), parts along dimension 0, may hold values from -0.75 to 0.75
- norm_gain: bfloat16 [7168], P('kv'), may hold values from 0.5 to 1.5
- expert_ids: int32 [80, 8], P('groups'), parts along dimension 0, may hold values from 0 to 255, all different within a row; in each aligned block of 40 rows (0 to 39, 40 to 79, ...) at most 2 rows name the same one
- gate_weights: float32 [80, 8], P('groups'), parts along dimension 0, may hold values from 0.05 to 0.5
Outputs:
- dispatched: bfloat16 [512, 2, 7168], P(('groups', 'kv')), parts along dimension 0
- slot_scale: float32 [512, 2], P(('groups', 'kv')), parts along dimension 0
- slot_gate: float32 [512, 2], P(('groups', 'kv')), parts along dimension 0
The draws below stay inside these ranges and needn't reach their ends.
There are 2 independent parts, one for each index of `groups`. The reference program is written for one: setup_inputs(seed, part) draws one part's arguments, and reference() takes and returns one part's arrays. A program takes and returns all parts, laid end to end along the dimension named above; an argument that names none is the same for every part. Nothing has to cross between parts.
Inputs may be any that keep to these rules, and one draw needn't show every extreme that they name: `context_lengths`: multiples of 128; some sequence is 2048 long. `expert_ids`: each token names 8 different experts; no expert is named by more than 2 tokens, a bound that some block reaches.
All inputs are finite; a program needn't handle non-finite values. Where the reference program divides by a largest or mean magnitude, that divisor is 1e-20 or more.
Results may differ from the reference program's by a relative error of at most 0.0069.
Values may be sent and summed in bfloat16 or wider, within the bound.
A program may use at most 64 MiB of HBM per device.

```python
import math
import jax
import jax.numpy as jnp
import numpy as np
from jax import lax

H = 32
LAT = 512
ROPE = 64
VD = 128
D = 7168
EXPERTS = 256
TOPK = 8
SEQS = 40
CTX_DEV = 128
BLOCK = 128
CTX = 2048
CAP = 2
N_KV = 16


def draw_queries(key, part):
    base_key = jax.random.fold_in(jax.random.fold_in(key, 11), 0)
    values = jnp.clip(jax.random.normal(base_key, (SEQS, H, LAT + ROPE), jnp.float32), -6.0, 6.0)
    return values.reshape(SEQS, H * (LAT + ROPE)).astype(jnp.bfloat16)


def draw_context_lengths(key, part):
    count_key, pick_key = jax.random.split(jax.random.fold_in(key, 7))
    blocks = jax.random.randint(count_key, (SEQS,), 1, CTX // BLOCK + 1)
    longest = jax.random.randint(pick_key, (), 0, SEQS)
    blocks = jnp.where(jnp.arange(SEQS) == longest, CTX // BLOCK, blocks)
    return (blocks * BLOCK).astype(jnp.int32)


def level_of(key, shape, cuts, least, high):
    def one(axis_at, shards_of):
        steps = jax.random.uniform(jax.random.fold_in(jax.random.fold_in(key, 6), axis_at), (shards_of,), jnp.float32, least / len(cuts), high / len(cuts))
        return jnp.repeat(jnp.exp(steps), shape[axis_at] // shards_of).reshape((-1,) + (1,) * (len(shape) - axis_at - 1))

    level = one(*cuts[0])
    for cut in cuts[1:]:
        level = level * one(*cut)
    return level


def assign_block(rng, own, number, rows, number_of, top, limit, skew):
    ranking = jax.random.permutation(rng, number_of)
    heavy_load, ordinary = shares(number_of, rows * top, limit, skew, True), shares(number_of, rows * top, limit, skew, False)
    places = jnp.arange(number_of)

    def named(lengths, rotation):
        used = int((lengths > 0).sum())
        fixed = max(1, used // 4)
        moved = fixed + (places - fixed + rotation * (used - fixed)) % max(1, number_of - fixed)
        return jnp.zeros((number_of,), jnp.int32).at[ranking[jnp.where(places < fixed, places, moved)]].set(jnp.asarray(lengths, jnp.int32))

    lengths = jnp.where(number % 4 == 0, named(heavy_load, number // 4), named(ordinary, number - number // 4 - 1))
    mixed = jax.random.permutation(jax.random.fold_in(own, 3), number_of)
    giver, sink = mixed[0:number_of // 2 * 2:2], mixed[1:number_of // 2 * 2:2]
    margin = jnp.minimum(lengths[giver] - 1, limit - lengths[sink]) // 2
    margin = jnp.where((giver == ranking[0]) | (sink == ranking[0]) | (lengths[sink] == 0), 0, jnp.maximum(margin, 0))
    moved = jax.random.randint(jax.random.fold_in(own, 4), (number_of // 2,), 0, 1 << 20) % (margin + 1)
    lengths = lengths.at[giver].add(-moved).at[sink].add(moved)
    labels = jnp.searchsorted(jnp.cumsum(lengths), jnp.arange(rows * top), side="right").astype(jnp.int32)
    listing = labels.reshape(top, rows).T
    listing = listing[jax.random.permutation(jax.random.fold_in(own, 1), rows)]
    rotation = jax.random.randint(jax.random.fold_in(own, 2), (rows, 1), 0, top)
    return jnp.take_along_axis(listing, (jnp.arange(top)[None, :] + rotation) % top, axis=1)


def shares(count, total, most, skew, full):
    loads = [(1 << 20) // math.isqrt(grade ** skew) + 1 for grade in range(1, count + 1)]
    largest = most if full else min(most, max(-(-total // count), total * loads[0] // sum(loads)))
    least = 1 if total - largest >= count - 1 else 0
    holding, rest = [largest] + [least] * (count - 1), total - largest - least * (count - 1)
    while rest > 0:
        candidates = [i for i in range(1, count) if holding[i] < largest] or [i for i in range(1, count) if holding[i] < most]
        whole, left = sum([loads[i] for i in candidates]), rest
        for i in candidates:
            addition = min(most - holding[i], max(1, left * loads[i] // whole), rest)
            holding[i] = holding[i] + addition
            rest = rest - addition
    return np.array(holding)


def gaussian(stream_key, extent, scale, reach, cuts=(), held_as=jnp.bfloat16):
    loudness = level_of(stream_key, extent, cuts, -0.22, 0.18) if cuts else 1.0
    entries = jax.random.normal(stream_key, extent, jnp.float32) * scale * loudness
    return jnp.minimum(jnp.maximum(entries, -reach), reach).astype(held_as)


def setup_inputs(seed: int = 0, part: int = 0) -> dict:
    key_list = jax.random.split(jax.random.key(seed), 10)
    part_splits = jax.random.split(jax.random.fold_in(key_list[9], part), 10)
    queries = draw_queries(jax.random.fold_in(jax.random.fold_in(key_list[9], part), 71), part)
    latent_cache = gaussian(part_splits[1], (SEQS, CTX, LAT + ROPE), 1.0, 6.0, ((1, 16),))
    context_lengths = draw_context_lengths(jax.random.fold_in(jax.random.fold_in(key_list[9], part), 71), part)
    value_up = gaussian(key_list[3], (H * LAT, VD), LAT ** -0.5, 0.25, ((0, 16),))
    out_proj = gaussian(key_list[4], (H * VD, D), (H * VD) ** -0.5, 0.09375, ((0, 16),))
    residual = gaussian(part_splits[5], (SEQS, D), 0.05, 0.75, ((1, 16),))
    norm_gain = jnp.clip(1.0 + 0.1 * jax.random.normal(key_list[6], (D,), jnp.float32), 0.5, 1.5).astype(jnp.bfloat16)
    expert_ids_keys = jax.random.split(jax.random.fold_in(part_splits[7], 1), SEQS // SEQS)
    expert_ids_turns = jax.random.permutation(jax.random.fold_in(part_splits[7], 3), SEQS // SEQS)
    expert_ids = jax.vmap(lambda own, number: assign_block(jax.random.fold_in(part_splits[7], 2), own, number, SEQS, EXPERTS, TOPK, CAP, 2))(expert_ids_keys, expert_ids_turns).reshape((SEQS, TOPK))
    gate_weights = jnp.clip(jax.random.uniform(part_splits[8], (SEQS, TOPK), jnp.float32, 0.05, 0.5), 0.05, 0.5)
    return dict(queries=queries, latent_cache=latent_cache, context_lengths=context_lengths, value_up=value_up, out_proj=out_proj, residual=residual, norm_gain=norm_gain, expert_ids=expert_ids, gate_weights=gate_weights)


score_scale = 192.0 ** (-0.5)
masked_score = -1e+30
small_eps = 1e-06

def slot_targets(expert_ids):
    flat_ids = expert_ids.reshape(-1).astype(jnp.int32)
    order_index = jnp.arange(flat_ids.shape[0], dtype=jnp.int32)
    same_before = (flat_ids[:, None] == flat_ids[None, :]) & (order_index[None, :] < order_index[:, None])
    rank_within = lax.optimization_barrier(jnp.sum(same_before.astype(jnp.int32), axis=1)).astype(jnp.int32)
    return flat_ids * CAP + rank_within

def reference(queries, latent_cache, context_lengths, value_up, out_proj, residual, norm_gain, expert_ids, gate_weights):
    query_rows = queries.reshape(SEQS, H, LAT + ROPE).astype(jnp.float32)
    shards = latent_cache.reshape(SEQS, N_KV, CTX_DEV, LAT + ROPE)

    def shard_step(running, shard_index):
        run_max, run_total, run_out = running
        cache_block = lax.dynamic_index_in_dim(shards, shard_index, 1, keepdims=False).astype(jnp.float32)
        scores = jnp.einsum('shq,scq->shc', query_rows, cache_block, precision=lax.Precision.HIGHEST) * score_scale
        position = shard_index * CTX_DEV + jnp.arange(CTX_DEV, dtype=jnp.int32)
        valid_mask = (position[None, :] < context_lengths[:, None])[:, None, :]
        scores = jnp.where(valid_mask, scores, masked_score)
        local_max = lax.optimization_barrier(jnp.max(scores, axis=2))
        weights = jnp.where(valid_mask, jnp.exp(scores - local_max[:, :, None]), 0.0)
        local_total = lax.optimization_barrier(jnp.sum(weights, axis=2))
        rounded = lax.optimization_barrier(weights.astype(jnp.bfloat16)).astype(jnp.float32)
        local_out = jnp.einsum('shc,scl->shl', rounded, cache_block[:, :, :LAT], precision=lax.Precision.HIGHEST)
        new_max = jnp.maximum(run_max, local_max)
        old_scale = jnp.exp(run_max - new_max)
        new_scale = jnp.exp(local_max - new_max)
        run_total = run_total * old_scale + local_total * new_scale
        run_out = run_out * old_scale[:, :, None] + local_out * new_scale[:, :, None]
        return ((new_max, run_total, run_out), None)
    start_state = (jnp.full((SEQS, H), masked_score, jnp.float32), jnp.zeros((SEQS, H), jnp.float32), jnp.zeros((SEQS, H, LAT), jnp.float32))
    final_state, unused = lax.scan(shard_step, start_state, jnp.arange(N_KV, dtype=jnp.int32))
    run_max, run_total, run_out = final_state
    merged = run_out / run_total[:, :, None]
    projector = value_up.reshape(H, LAT, VD).astype(jnp.float32)
    value_part = jnp.einsum('shl,hlv->shv', merged, projector, precision=lax.Precision.HIGHEST)
    value_rows = value_part.astype(jnp.bfloat16).reshape(SEQS, H * VD)
    attn_rows = jnp.dot(value_rows, out_proj, preferred_element_type=jnp.float32)
    summed = attn_rows + residual.astype(jnp.float32)
    inverse_rms = lax.rsqrt(lax.optimization_barrier(jnp.mean(summed * summed, axis=1)) + small_eps)
    normed = summed * inverse_rms[:, None] * norm_gain.astype(jnp.float32)
    peak_abs = lax.optimization_barrier(jnp.max(jnp.abs(normed), axis=1)) + small_eps
    coded_rows = (normed / peak_abs[:, None]).astype(jnp.bfloat16)
    targets = slot_targets(expert_ids)
    owner = jnp.arange(SEQS * TOPK, dtype=jnp.int32) // TOPK
    dispatched = jnp.zeros((EXPERTS * CAP, D), jnp.bfloat16).at[targets].set(coded_rows[owner])
    slot_scale = jnp.zeros((EXPERTS * CAP,), jnp.float32).at[targets].set(peak_abs[owner])
    slot_gate = jnp.zeros((EXPERTS * CAP,), jnp.float32).at[targets].set(gate_weights.reshape(-1))
    return (dispatched.reshape(EXPERTS, CAP, D), slot_scale.reshape(EXPERTS, CAP), slot_gate.reshape(EXPERTS, CAP))
```

```python
import functools

import jax
import jax.numpy as jnp
from jax import lax
from jax.experimental import pallas as pl
from jax.experimental.pallas import tpu as pltpu
from jax.sharding import PartitionSpec as P

H = 32
LAT = 512
ROPE = 64
VD = 128
D = 7168
EXPERTS = 256
TOPK = 8
CAP = 2


score_scale = 192.0 ** (-0.5)
masked_score = -1e30
small_eps = 1e-06


def from_partner(value, axis, bit):
    mask = 2**bit
    pairs = [(source, source ^ mask) for source in range(lax.axis_size(axis))]
    return lax.ppermute(value, axis, pairs)


def slot_targets(expert_ids):
    flat_ids = expert_ids.reshape(-1)
    order_index = jnp.arange(flat_ids.shape[0], dtype=jnp.int32)
    same_before = (flat_ids[:, None] == flat_ids[None, :]) & (
        order_index[None, :] < order_index[:, None]
    )
    rank_within = jnp.sum(same_before.astype(jnp.int32), axis=1)
    return flat_ids * CAP + rank_within


def slot_match(targets, first_slot, slot_count):
    slot_index = first_slot + jnp.arange(slot_count, dtype=jnp.int32)
    return (slot_index[:, None] == targets[None, :]).astype(jnp.float32)


def token_picker(matches, seq_count):
    return jnp.sum(matches.reshape(matches.shape[0], seq_count, TOPK), axis=2)


def general_device(
    queries,
    latent_cache,
    context_lengths,
    value_up,
    out_proj,
    residual,
    norm_gain,
    expert_ids,
    gate_weights,
):
    kv_count = lax.axis_size("kv")
    shard_index = lax.axis_index("kv")
    seq_count = queries.shape[0]
    query_rows = lax.all_gather(queries, "kv", axis=1, tiled=True).reshape(seq_count, H, LAT + ROPE)
    ctx_local = latent_cache.shape[1]
    scores = (
        jnp.einsum("shq,scq->shc", query_rows, latent_cache, preferred_element_type=jnp.float32)
        * score_scale
    )
    position = shard_index * ctx_local + jnp.arange(ctx_local, dtype=jnp.int32)
    valid_mask = (position[None, :] < context_lengths[:, None])[:, None, :]
    scores = jnp.where(valid_mask, scores, masked_score)
    local_max = jnp.max(scores, axis=2)
    weights = jnp.where(valid_mask, jnp.exp(scores - local_max[:, :, None]), 0.0)
    local_total = jnp.sum(weights, axis=2)
    local_out = jnp.einsum(
        "shc,scl->shl",
        weights.astype(jnp.bfloat16),
        latent_cache[:, :, :LAT],
        preferred_element_type=jnp.float32,
    )
    out_rows = out_proj.shape[0]
    col_count = H * LAT // kv_count
    segment = min(col_count, LAT)
    head_count = col_count // segment
    head_start = shard_index * col_count // LAT
    global_max = lax.pmax(local_max, "kv")
    scaling = jnp.exp(local_max - global_max)
    weight_total = lax.psum(local_total * scaling, "kv")
    scaled = (local_out * scaling[:, :, None]).reshape(seq_count, H * LAT)
    merged_sum = lax.psum_scatter(scaled, "kv", scatter_dimension=1, tiled=True).reshape(
        seq_count, head_count, segment
    )
    own_total = lax.dynamic_slice_in_dim(weight_total, head_start, head_count, 1)
    merged = merged_sum / own_total[:, :, None]
    projector = value_up.reshape(head_count, segment, VD).astype(jnp.float32)
    value_part = jnp.einsum("shl,hlv->shv", merged, projector, precision=lax.Precision.HIGHEST)
    holders = kv_count // H if kv_count > H else 1
    for bit in range(holders.bit_length() - 1):
        value_part = value_part + from_partner(value_part, "kv", bit)
    value_rows = value_part.astype(jnp.bfloat16).reshape(seq_count, head_count * VD)
    if holders > 1:
        value_rows = lax.dynamic_slice_in_dim(
            value_rows, shard_index % holders * out_rows, out_rows, 1
        )
    partial_out = jnp.dot(value_rows, out_proj, preferred_element_type=jnp.float32)
    experts_local = EXPERTS // kv_count
    slot_count = experts_local * CAP
    targets = slot_targets(expert_ids)
    own_match = slot_match(targets, shard_index * slot_count, slot_count)
    own_pick = token_picker(own_match, seq_count)
    slot_gate = jnp.dot(own_match, gate_weights.reshape(-1), precision=lax.Precision.HIGHEST)
    attn_rows = lax.psum(partial_out, "kv")
    resid_rows, gain_cols = (
        lax.all_gather(residual, "kv", axis=1, tiled=True),
        lax.all_gather(norm_gain, "kv", axis=0, tiled=True),
    )
    summed = attn_rows + resid_rows.astype(jnp.float32)
    inverse_rms = lax.rsqrt(jnp.mean(summed * summed, axis=1) + small_eps)
    normed = summed * inverse_rms[:, None] * gain_cols.astype(jnp.float32)
    peak_abs = jnp.max(jnp.abs(normed), axis=1) + small_eps
    coded_rows = (normed / peak_abs[:, None]).astype(jnp.bfloat16)
    dispatched = jnp.dot(
        own_pick.astype(jnp.bfloat16), coded_rows, preferred_element_type=jnp.float32
    ).astype(jnp.bfloat16)
    slot_scale = jnp.dot(own_pick, peak_abs, precision=lax.Precision.HIGHEST)
    return (
        dispatched.reshape(experts_local, CAP, D),
        slot_scale.reshape(experts_local, CAP),
        slot_gate.reshape(experts_local, CAP),
    )


CORES = 2
LINKED_Y = 2
LANES = 128
ROWS = 8
F32 = jnp.float32
BF16 = jnp.bfloat16


def split3(value):
    first = value.astype(BF16).astype(F32)
    rest = value - first
    second = rest.astype(BF16).astype(F32)
    return first, second, rest - second


def put_lanes(shape, columns):
    lane = lax.broadcasted_iota(jnp.int32, shape, len(shape) - 1)
    tile = jnp.zeros(shape, F32)
    for index, column in columns:
        tile = jnp.where(lane == index, column, tile)
    return tile


def take3(tile, start):
    return (
        tile[..., start : start + 1]
        + tile[..., start + 1 : start + 2]
        + tile[..., start + 2 : start + 3]
    )


def merge(blocks):
    heads = (blocks[0].shape[-1] - LANES) // LAT
    outs, columns = [], []
    for head in range(heads):
        stats = [block[..., heads * LAT :] for block in blocks]
        maxes = [take3(stat, head * 6) for stat in stats]
        totals = [take3(stat, head * 6 + 3) for stat in stats]
        top = maxes[0]
        for other in maxes[1:]:
            top = jnp.maximum(top, other)
        total, out = 0.0, 0.0
        for block, own_max, own_total in zip(blocks, maxes, totals):
            factor = jnp.exp(own_max - top)
            total = total + factor * own_total
            out = out + factor * block[..., head * LAT : (head + 1) * LAT]
        outs.append((out, top, total))
    return outs


def message(outs):
    columns = []
    for head, (out, top, total) in enumerate(outs):
        for index, part in enumerate(split3(top) + split3(total)):
            columns.append((head * 6 + index, part))
    shape = outs[0][0].shape[:-1] + (LANES,)
    return jnp.concatenate([out for out, _, _ in outs] + [put_lanes(shape, columns)], axis=-1)


def step_kernel(
    zs,
    chunks,
    q_ref,
    cache_hbm,
    ctx_ref,
    up_ref,
    proj_hbm,
    resid_ref,
    gain_ref,
    pick_ref,
    out_ref,
    scale_ref,
    cache,
    proj,
    qbuf,
    qrow,
    osc,
    msc,
    s1,
    r1,
    k1,
    r2,
    k2,
    r3,
    merged,
    part,
    ps1,
    pr1,
    pk1,
    pr2,
    pk2,
    pr3,
    gbuf,
    gainbuf,
    load_sem,
    proj_sem,
    qz_s,
    qz_r,
    q_s,
    q_r,
    oz_s,
    oz_r,
    o_s,
    o_r,
    pz_s,
    pz_r,
    p_s,
    p_r,
):
    me = lax.axis_index("kv")
    core = lax.rem(me, CORES)
    y = lax.rem(me // CORES, LINKED_Y)
    z = me // (CORES * LINKED_Y)

    def device(zz, yy, cc):
        return {"kv": (zz * LINKED_Y + yy) * CORES + cc}

    partner = device(z, y, 1 - core)
    across = device(z, 1 - y, core)
    along = [lax.rem(z + step, zs) for step in range(1, zs)]
    back = [lax.rem(z + zs - step, zs) for step in range(1, zs)]

    def copy(source, target, send, recv, where):
        return pltpu.make_async_remote_copy(
            src_ref=source,
            dst_ref=target,
            send_sem=send,
            recv_sem=recv,
            device_id=where,
            device_id_type=pl.DeviceIdType.MESH,
        )

    loads = [
        pltpu.make_async_copy(
            cache_hbm.at[pl.ds(k * ROWS, ROWS)], cache.at[pl.ds(k * ROWS, ROWS)], load_sem.at[k]
        )
        for k in range(chunks)
    ]
    for load in loads:
        load.start()
    proj_load = pltpu.make_async_copy(proj_hbm, proj, proj_sem)
    proj_load.start()

    barrier = pltpu.get_barrier_semaphore()
    peers = [partner, across] + [device(zz, y, core) for zz in along]
    for peer in peers:
        pl.semaphore_signal(
            barrier, inc=1, device_id=peer, device_id_type=pl.DeviceIdType.MESH
        )
    pl.semaphore_wait(barrier, len(peers))

    pending = []

    def z_copies(source_of, target, send, recv):
        made = []
        for step, zz in enumerate(along):
            made.append(copy(source_of(zz), target, send.at[step], recv.at[step], device(zz, y, core)))
        return made

    def launch(made):
        for one in made:
            one.start()
            pending.append(one)
        return made

    gain_copy = launch(
        [copy(gain_ref, gainbuf, p_s.at[4], p_r.at[4], partner)]
    )
    q_along = [
        launch(z_copies(lambda zz: q_ref.at[k], qbuf.at[k, core, y, z], qz_s.at[k], qz_r.at[k]))
        for k in range(chunks)
    ]
    for k in range(chunks):
        qbuf[k, core, y, z] = q_ref[k]
    q_across, q_pair, o_pair, o_across, o_along = {}, {}, {}, {}, {}

    def gather_across(k):
        for one in q_along[k]:
            one.wait_recv()
        q_across[k] = launch(
            [copy(qbuf.at[k, core, y], qbuf.at[k, core, y], q_s.at[k, 0], q_r.at[k, 0], across)]
        )

    def gather_pair(k):
        q_across[k][0].wait_recv()
        q_pair[k] = launch(
            [copy(qbuf.at[k, core], qbuf.at[k, core], q_s.at[k, 1], q_r.at[k, 1], partner)]
        )

    ctx_local = cache.shape[1]
    count = CORES * LINKED_Y * zs
    position = me * ctx_local + lax.broadcasted_iota(jnp.int32, (2 * count, ctx_local), 1)

    def attend(k):
        q_pair[k][0].wait_recv()
        loads[k].wait()
        width = q_ref.shape[-1]
        rows = qbuf[k].reshape(count, ROWS, width).astype(F32)
        qrow[...] = jnp.swapaxes(rows, 0, 1).astype(BF16)

        def one(s, carry):
            row = qrow[s]
            keys = cache[k * ROWS + s]
            latent = jnp.concatenate([row[:, :LAT], row[:, LAT : 2 * LAT]], axis=0)
            rotary = row[:, 2 * LAT :]
            rotary = jnp.concatenate([rotary[:, :ROPE], rotary[:, ROPE:]], axis=0)
            over = (((1,), (1,)), ((), ()))
            scores = lax.dot_general(latent, keys[:, :LAT], over, preferred_element_type=F32)
            scores = scores + lax.dot_general(
                rotary, keys[:, LAT:], over, preferred_element_type=F32
            )
            valid = position < ctx_ref[k * ROWS + s]
            scores = jnp.where(valid, scores * score_scale, masked_score)
            top = jnp.max(scores, axis=1, keepdims=True)
            weights = jnp.where(valid, jnp.exp(scores - top), 0.0)
            total = jnp.sum(weights, axis=1, keepdims=True)
            osc[s] = jnp.dot(weights.astype(BF16), keys[:, :LAT], preferred_element_type=F32)
            columns = []
            for head in range(2):
                here = slice(head * count, (head + 1) * count)
                parts = split3(top[here]) + split3(total[here])
                columns += [(head * 6 + index, value) for index, value in enumerate(parts)]
            msc[s] = put_lanes((count, LANES), columns)
            return carry

        lax.fori_loop(0, ROWS, one, 0)
        whole = jnp.swapaxes(osc[...], 0, 1).astype(BF16)
        shape = (CORES, LINKED_Y, zs, ROWS)
        s1[k, :, :, :, :, :LAT] = whole[:count].reshape(shape + (LAT,))
        s1[k, :, :, :, :, LAT : 2 * LAT] = whole[count:].reshape(shape + (LAT,))
        s1[k, :, :, :, :, 2 * LAT :] = (
            jnp.swapaxes(msc[...], 0, 1).astype(BF16).reshape(shape + (LANES,))
        )
        o_pair[k] = launch([copy(s1.at[k, 1 - core], r1.at[k], o_s.at[k, 0], o_r.at[k, 0], partner)])

    def merge_pair(k):
        o_pair[k][0].wait_recv()

        def one(i, carry):
            k1[k, 1 - y, i] = message(
                merge([s1[k, core, 1 - y, i].astype(F32), r1[k, 1 - y, i].astype(F32)])
            ).astype(BF16)
            return carry

        lax.fori_loop(0, zs, one, 0)
        o_across[k] = launch([copy(k1.at[k, 1 - y], r2.at[k], o_s.at[k, 1], o_r.at[k, 1], across)])

    def merge_across(k):
        o_across[k][0].wait_recv()

        def one(i, carry):
            k2[k, i] = message(
                merge(
                    [
                        s1[k, core, y, i].astype(F32),
                        r1[k, y, i].astype(F32),
                        r2[k, i].astype(F32),
                    ]
                )
            ).astype(BF16)
            return carry

        lax.fori_loop(0, zs, one, 0)
        o_along[k] = launch(
            [
                copy(k2.at[k, zz], r3.at[k, step], oz_s.at[k, step], oz_r.at[k, step], device(zz, y, core))
                for step, zz in enumerate(along)
            ]
        )

    def merge_along(k):
        for one in o_along[k]:
            one.wait_recv()
        blocks = [k2[k, z].astype(F32)] + [r3[k, step].astype(F32) for step in range(zs - 1)]
        for head, (out, _, total) in enumerate(merge(blocks)):
            merged[head, pl.ds(k * ROWS, ROWS), :] = out / total

    for t in range(chunks + 5):
        for stage, lag in (
            (gather_across, 0),
            (gather_pair, 1),
            (attend, 2),
            (merge_pair, 3),
            (merge_across, 4),
            (merge_along, 5),
        ):
            if 0 <= t - lag < chunks:
                stage(t - lag)

    values = []
    for head in range(2):
        own = merged[head]
        high = own.astype(BF16)
        low = (own - high.astype(F32)).astype(BF16)
        rows = up_ref[head * LAT : (head + 1) * LAT]
        values.append(
            jnp.dot(high, rows, preferred_element_type=F32)
            + jnp.dot(low, rows, preferred_element_type=F32)
        )
    value = jnp.concatenate(values, axis=1).astype(BF16)
    proj_load.wait()
    chip_cols = part.shape[-1]
    held = ps1.shape[-1]
    skip = chip_cols - held
    for zz in range(zs):
        for yy in range(LINKED_Y):
            start = (zz * LINKED_Y + yy) * chip_cols
            part[yy, zz] = jnp.dot(
                value, proj[:, start : start + chip_cols], preferred_element_type=F32
            )
    part[y, z] = part[y, z] + resid_ref[...].astype(F32)
    own_cols = pl.ds(pl.multiple_of(core * skip, LANES), held)
    other_cols = pl.ds(pl.multiple_of((1 - core) * skip, LANES), held)
    ps1[...] = part[:, :, :, other_cols].astype(BF16)
    p_pair = launch([copy(ps1, pr1, p_s.at[0], p_r.at[0], partner)])
    p_pair[0].wait_recv()
    pk1[...] = (part[1 - y, :, :, own_cols] + pr1[1 - y].astype(F32)).astype(BF16)
    p_across = launch([copy(pk1, pr2, p_s.at[1], p_r.at[1], across)])
    p_across[0].wait_recv()
    kept = part[y, :, :, own_cols] + pr1[y].astype(F32) + pr2[...].astype(F32)
    part[y, :, :, own_cols] = kept
    pk2[...] = kept.astype(BF16)
    p_along = launch(
        [
            copy(pk2.at[zz], pr3.at[step], pz_s.at[0, step], pz_r.at[0, step], device(zz, y, core))
            for step, zz in enumerate(along)
        ]
    )
    gain_copy[0].wait_recv()
    for one in p_along:
        one.wait_recv()
    summed = part[y, z, :, own_cols]
    for step in range(zs - 1):
        summed = summed + pr3[step].astype(F32)
    gain = (gain_ref[...].astype(F32) + gainbuf[...].astype(F32))[:1]
    gain = jnp.where(core == 0, gain[:, :held], gain[:, skip:])
    scaled = summed * gain
    lane = lax.broadcasted_iota(jnp.int32, summed.shape, 1)
    first = jnp.where(core == 0, 0, 2 * held - chip_cols)
    square = jnp.sum(jnp.where(lane >= first, summed * summed, 0.0), axis=1, keepdims=True)
    largest = jnp.max(jnp.abs(scaled), axis=1, keepdims=True)
    columns = list(enumerate(split3(square) + split3(largest)))
    stats = put_lanes((summed.shape[0], LANES), columns)
    gbuf[core, y, z] = jnp.concatenate([scaled, stats], axis=1).astype(BF16)
    g_along = launch(
        [
            copy(
                gbuf.at[core, y, z],
                gbuf.at[core, y, z],
                pz_s.at[1, step],
                pz_r.at[1, step],
                device(zz, y, core),
            )
            for step, zz in enumerate(along)
        ]
    )
    for one in g_along:
        one.wait_recv()
    g_across = launch([copy(gbuf.at[core, y], gbuf.at[core, y], p_s.at[2], p_r.at[2], across)])
    g_across[0].wait_recv()
    g_pair = launch([copy(gbuf.at[core], gbuf.at[core], p_s.at[3], p_r.at[3], partner)])
    g_pair[0].wait_recv()

    stats = gbuf[:, :, :, :, held:].astype(F32).reshape(count, summed.shape[0], LANES)
    square = jnp.sum(take3(stats, 0), axis=0)
    largest = jnp.max(take3(stats, 3), axis=0)
    inverse = lax.rsqrt(square / (chip_cols * LINKED_Y * zs) + small_eps)
    peak = largest * inverse + small_eps
    factor = inverse / peak
    pick = pick_ref[...].astype(BF16)
    for zz in range(zs):
        for yy in range(LINKED_Y):
            start = (zz * LINKED_Y + yy) * chip_cols
            for cc in range(CORES):
                drop = cc * (2 * held - chip_cols)
                rows = gbuf[cc, yy, zz, :, drop:held].astype(F32) * factor
                at = start + cc * held
                out_ref[:, at : at + held - drop] = jnp.dot(
                    pick, rows.astype(BF16), preferred_element_type=F32
                ).astype(BF16)
    scale_ref[...] = jnp.dot(
        pick_ref[...],
        jnp.broadcast_to(peak, (peak.shape[0], LANES)),
        precision=lax.Precision.HIGHEST,
        preferred_element_type=F32,
    )
    for one in pending:
        one.wait_send()


def fused_device(
    queries,
    latent_cache,
    context_lengths,
    value_up,
    out_proj,
    residual,
    norm_gain,
    expert_ids,
    gate_weights,
):
    kv_count = lax.axis_size("kv")
    shard_index = lax.axis_index("kv")
    core = shard_index % CORES
    zs = kv_count // (CORES * LINKED_Y)
    seq_count = queries.shape[0]
    chunks = seq_count // ROWS
    ctx_local = latent_cache.shape[1]
    width = queries.shape[1]
    cols = residual.shape[1]
    chip_cols = cols * CORES
    held = -(-cols // LANES) * LANES
    heads = queries.reshape(seq_count, H // kv_count, LAT + ROPE)
    rows = jnp.concatenate(
        [heads[:, :, :LAT].reshape(seq_count, -1), heads[:, :, LAT:].reshape(seq_count, -1)], axis=1
    ).reshape(chunks, ROWS, width)

    def placed(block):
        zero = jnp.zeros_like(block)
        return jnp.concatenate(
            [jnp.where(core == 0, block, zero), jnp.where(core == 0, zero, block)], axis=1
        )

    gain = placed(jnp.broadcast_to(norm_gain[None, :], (ROWS, cols)))
    experts_local = EXPERTS // kv_count
    slot_count = experts_local * CAP
    targets = slot_targets(expert_ids)
    own_match = slot_match(targets, shard_index * slot_count, slot_count)
    own_pick = token_picker(own_match, seq_count)
    slot_gate = jnp.sum(own_match * gate_weights.reshape(1, -1), axis=1)

    vmem = pl.BlockSpec(memory_space=pltpu.VMEM)
    smem = pl.BlockSpec(memory_space=pltpu.SMEM)
    anywhere = pl.BlockSpec(memory_space=pl.ANY)
    dma = pltpu.SemaphoreType.DMA
    full = (LINKED_Y, zs)
    dispatched, scale = pl.pallas_call(
        functools.partial(step_kernel, zs, chunks),
        out_shape=(
            jax.ShapeDtypeStruct((slot_count, chip_cols * LINKED_Y * zs), BF16),
            jax.ShapeDtypeStruct((slot_count, LANES), F32),
        ),
        in_specs=[vmem, anywhere, smem, vmem, anywhere, vmem, vmem, vmem],
        out_specs=(vmem, vmem),
        scratch_shapes=[
            pltpu.VMEM(latent_cache.shape, BF16),
            pltpu.VMEM(out_proj.shape, BF16),
            pltpu.VMEM((chunks, CORES) + full + (ROWS, width), BF16),
            pltpu.VMEM((ROWS, kv_count, width), BF16),
            pltpu.VMEM((ROWS, H, LAT), F32),
            pltpu.VMEM((ROWS, kv_count, LANES), F32),
            pltpu.VMEM((chunks, CORES) + full + (ROWS, width), BF16),
            pltpu.VMEM((chunks,) + full + (ROWS, width), BF16),
            pltpu.VMEM((chunks,) + full + (ROWS, width), BF16),
            pltpu.VMEM((chunks, zs, ROWS, width), BF16),
            pltpu.VMEM((chunks, zs, ROWS, width), BF16),
            pltpu.VMEM((chunks, zs - 1, ROWS, width), BF16),
            pltpu.VMEM((H // kv_count, seq_count, LAT), F32),
            pltpu.VMEM(full + (seq_count, chip_cols), F32),
            pltpu.VMEM(full + (seq_count, held), BF16),
            pltpu.VMEM(full + (seq_count, held), BF16),
            pltpu.VMEM((zs, seq_count, held), BF16),
            pltpu.VMEM((zs, seq_count, held), BF16),
            pltpu.VMEM((zs, seq_count, held), BF16),
            pltpu.VMEM((zs - 1, seq_count, held), BF16),
            pltpu.VMEM((CORES,) + full + (seq_count, held + LANES), BF16),
            pltpu.VMEM((ROWS, chip_cols), BF16),
            dma((chunks,)),
            dma,
            dma((chunks, zs - 1)),
            dma((chunks, zs - 1)),
            dma((chunks, 2)),
            dma((chunks, 2)),
            dma((chunks, zs - 1)),
            dma((chunks, zs - 1)),
            dma((chunks, 2)),
            dma((chunks, 2)),
            dma((2, zs - 1)),
            dma((2, zs - 1)),
            dma((5,)),
            dma((5,)),
        ],
        compiler_params=pltpu.CompilerParams(
            collective_id=0, has_side_effects=True, vmem_limit_bytes=60 * 1024 * 1024
        ),
    )(
        rows,
        latent_cache,
        context_lengths,
        value_up,
        out_proj,
        placed(residual),
        gain,
        own_pick,
    )
    return (
        dispatched.reshape(experts_local, CAP, -1),
        scale[:, 0].reshape(experts_local, CAP),
        slot_gate.reshape(experts_local, CAP),
    )


def per_device(*arrays):
    queries, residual = arrays[0], arrays[5]
    kv_count = lax.axis_size("kv")
    pairs = H == 2 * kv_count and 2 * ROPE == LANES and kv_count % (CORES * LINKED_Y) == 0
    aligned = queries.shape[0] % ROWS == 0 and residual.shape[1] * CORES % LANES == 0
    if pairs and aligned:
        return fused_device(*arrays)
    return general_device(*arrays)


def solution(mesh):
    in_specs = (
        P("groups", "kv"),
        P("groups", "kv", None),
        P("groups"),
        P("kv", None),
        P("kv", None),
        P("groups", "kv"),
        P("kv"),
        P("groups", None),
        P("groups", None),
    )
    out_specs = (
        P(("groups", "kv"), None, None),
        P(("groups", "kv"), None),
        P(("groups", "kv"), None),
    )
    return jax.shard_map(
        per_device, mesh=mesh, in_specs=in_specs, out_specs=out_specs, check_vma=False
    )
```

```python
import functools

import jax
import jax.numpy as jnp
from jax import lax
from jax.experimental import pallas as pl
from jax.experimental.pallas import tpu as pltpu
from jax.sharding import PartitionSpec as P

H = 32
LAT = 512
ROPE = 64
VD = 128
D = 7168
EXPERTS = 256
TOPK = 8
CAP = 2


score_scale = 192.0 ** (-0.5)
masked_score = -1e30
small_eps = 1e-06


def from_partner(value, axis, bit):
    mask = 2**bit
    pairs = [(source, source ^ mask) for source in range(lax.axis_size(axis))]
    return lax.ppermute(value, axis, pairs)


def slot_targets(expert_ids):
    flat_ids = expert_ids.reshape(-1)
    order_index = jnp.arange(flat_ids.shape[0], dtype=jnp.int32)
    same_before = (flat_ids[:, None] == flat_ids[None, :]) & (
        order_index[None, :] < order_index[:, None]
    )
    rank_within = jnp.sum(same_before.astype(jnp.int32), axis=1)
    return flat_ids * CAP + rank_within


def slot_match(targets, first_slot, slot_count):
    slot_index = first_slot + jnp.arange(slot_count, dtype=jnp.int32)
    return (slot_index[:, None] == targets[None, :]).astype(jnp.float32)


def token_picker(matches, seq_count):
    return jnp.sum(matches.reshape(matches.shape[0], seq_count, TOPK), axis=2)


def general_device(
    queries,
    latent_cache,
    context_lengths,
    value_up,
    out_proj,
    residual,
    norm_gain,
    expert_ids,
    gate_weights,
):
    kv_count = lax.axis_size("kv")
    shard_index = lax.axis_index("kv")
    seq_count = queries.shape[0]
    query_rows = lax.all_gather(queries, "kv", axis=1, tiled=True).reshape(seq_count, H, LAT + ROPE)
    ctx_local = latent_cache.shape[1]
    scores = (
        jnp.einsum("shq,scq->shc", query_rows, latent_cache, preferred_element_type=jnp.float32)
        * score_scale
    )
    position = shard_index * ctx_local + jnp.arange(ctx_local, dtype=jnp.int32)
    valid_mask = (position[None, :] < context_lengths[:, None])[:, None, :]
    scores = jnp.where(valid_mask, scores, masked_score)
    local_max = jnp.max(scores, axis=2)
    weights = jnp.where(valid_mask, jnp.exp(scores - local_max[:, :, None]), 0.0)
    local_total = jnp.sum(weights, axis=2)
    local_out = jnp.einsum(
        "shc,scl->shl",
        weights.astype(jnp.bfloat16),
        latent_cache[:, :, :LAT],
        preferred_element_type=jnp.float32,
    )
    out_rows = out_proj.shape[0]
    col_count = H * LAT // kv_count
    segment = min(col_count, LAT)
    head_count = col_count // segment
    head_start = shard_index * col_count // LAT
    global_max = lax.pmax(local_max, "kv")
    scaling = jnp.exp(local_max - global_max)
    weight_total = lax.psum(local_total * scaling, "kv")
    scaled = (local_out * scaling[:, :, None]).reshape(seq_count, H * LAT)
    merged_sum = lax.psum_scatter(scaled, "kv", scatter_dimension=1, tiled=True).reshape(
        seq_count, head_count, segment
    )
    own_total = lax.dynamic_slice_in_dim(weight_total, head_start, head_count, 1)
    merged = merged_sum / own_total[:, :, None]
    projector = value_up.reshape(head_count, segment, VD).astype(jnp.float32)
    value_part = jnp.einsum("shl,hlv->shv", merged, projector, precision=lax.Precision.HIGHEST)
    holders = kv_count // H if kv_count > H else 1
    for bit in range(holders.bit_length() - 1):
        value_part = value_part + from_partner(value_part, "kv", bit)
    value_rows = value_part.astype(jnp.bfloat16).reshape(seq_count, head_count * VD)
    if holders > 1:
        value_rows = lax.dynamic_slice_in_dim(
            value_rows, shard_index % holders * out_rows, out_rows, 1
        )
    partial_out = jnp.dot(value_rows, out_proj, preferred_element_type=jnp.float32)
    experts_local = EXPERTS // kv_count
    slot_count = experts_local * CAP
    targets = slot_targets(expert_ids)
    own_match = slot_match(targets, shard_index * slot_count, slot_count)
    own_pick = token_picker(own_match, seq_count)
    slot_gate = jnp.dot(own_match, gate_weights.reshape(-1), precision=lax.Precision.HIGHEST)
    attn_rows = lax.psum(partial_out, "kv")
    resid_rows, gain_cols = (
        lax.all_gather(residual, "kv", axis=1, tiled=True),
        lax.all_gather(norm_gain, "kv", axis=0, tiled=True),
    )
    summed = attn_rows + resid_rows.astype(jnp.float32)
    inverse_rms = lax.rsqrt(jnp.mean(summed * summed, axis=1) + small_eps)
    normed = summed * inverse_rms[:, None] * gain_cols.astype(jnp.float32)
    peak_abs = jnp.max(jnp.abs(normed), axis=1) + small_eps
    coded_rows = (normed / peak_abs[:, None]).astype(jnp.bfloat16)
    dispatched = jnp.dot(
        own_pick.astype(jnp.bfloat16), coded_rows, preferred_element_type=jnp.float32
    ).astype(jnp.bfloat16)
    slot_scale = jnp.dot(own_pick, peak_abs, precision=lax.Precision.HIGHEST)
    return (
        dispatched.reshape(experts_local, CAP, D),
        slot_scale.reshape(experts_local, CAP),
        slot_gate.reshape(experts_local, CAP),
    )


CORES = 2
LINKED_Y = 2
LANES = 128
ROWS = 8
F32 = jnp.float32
BF16 = jnp.bfloat16


def split3(value):
    first = value.astype(BF16).astype(F32)
    rest = value - first
    second = rest.astype(BF16).astype(F32)
    return first, second, rest - second


def put_lanes(shape, columns):
    lane = lax.broadcasted_iota(jnp.int32, shape, len(shape) - 1)
    tile = jnp.zeros(shape, F32)
    for index, column in columns:
        tile = jnp.where(lane == index, column, tile)
    return tile


def take3(tile, start):
    return (
        tile[..., start : start + 1]
        + tile[..., start + 1 : start + 2]
        + tile[..., start + 2 : start + 3]
    )


def merge(blocks):
    heads = (blocks[0].shape[-1] - LANES) // LAT
    outs, columns = [], []
    for head in range(heads):
        stats = [block[..., heads * LAT :] for block in blocks]
        maxes = [take3(stat, head * 6) for stat in stats]
        totals = [take3(stat, head * 6 + 3) for stat in stats]
        top = maxes[0]
        for other in maxes[1:]:
            top = jnp.maximum(top, other)
        total, out = 0.0, 0.0
        for block, own_max, own_total in zip(blocks, maxes, totals):
            factor = jnp.exp(own_max - top)
            total = total + factor * own_total
            out = out + factor * block[..., head * LAT : (head + 1) * LAT]
        outs.append((out, top, total))
    return outs


def message(outs):
    columns = []
    for head, (out, top, total) in enumerate(outs):
        for index, part in enumerate(split3(top) + split3(total)):
            columns.append((head * 6 + index, part))
    shape = outs[0][0].shape[:-1] + (LANES,)
    return jnp.concatenate([out for out, _, _ in outs] + [put_lanes(shape, columns)], axis=-1)


def step_kernel(
    zs,
    chunks,
    q_ref,
    cache_hbm,
    ctx_ref,
    up_ref,
    proj_hbm,
    resid_ref,
    gain_ref,
    ids_ref,
    gates_ref,
    out_ref,
    scale_ref,
    qown,
    gainown,
    pick_scr,
    cache,
    proj,
    qbuf,
    qrow,
    osc,
    msc,
    s1,
    r1,
    k1,
    r2,
    k2,
    r3,
    merged,
    part,
    ps1,
    pr1,
    pk1,
    pr2,
    pk2,
    pr3,
    gbuf,
    gainbuf,
    load_sem,
    proj_sem,
    qz_s,
    qz_r,
    q_s,
    q_r,
    oz_s,
    oz_r,
    o_s,
    o_r,
    pz_s,
    pz_r,
    p_s,
    p_r,
):
    me = lax.axis_index("kv")
    core = lax.rem(me, CORES)
    y = lax.rem(me // CORES, LINKED_Y)
    z = me // (CORES * LINKED_Y)

    def device(zz, yy, cc):
        return {"kv": (zz * LINKED_Y + yy) * CORES + cc}

    partner = device(z, y, 1 - core)
    across = device(z, 1 - y, core)
    along = [lax.rem(z + step, zs) for step in range(1, zs)]
    back = [lax.rem(z + zs - step, zs) for step in range(1, zs)]

    def copy(source, target, send, recv, where):
        return pltpu.make_async_remote_copy(
            src_ref=source,
            dst_ref=target,
            send_sem=send,
            recv_sem=recv,
            device_id=where,
            device_id_type=pl.DeviceIdType.MESH,
        )

    loads = [
        pltpu.make_async_copy(
            cache_hbm.at[pl.ds(k * ROWS, ROWS)], cache.at[pl.ds(k * ROWS, ROWS)], load_sem.at[k]
        )
        for k in range(chunks)
    ]
    for load in loads:
        load.start()
    proj_load = pltpu.make_async_copy(proj_hbm, proj, proj_sem)
    proj_load.start()

    raw = q_ref[...].astype(F32)
    key = LAT + ROPE
    qown[...] = jnp.concatenate(
        [raw[..., :LAT], raw[..., key : key + LAT], raw[..., LAT:key], raw[..., key + LAT :]],
        axis=-1,
    ).astype(BF16)

    def placed(block):
        zero = jnp.zeros_like(block)
        return jnp.where(
            core == 0,
            jnp.concatenate([block, zero], axis=-1),
            jnp.concatenate([zero, block], axis=-1),
        )

    gainown[...] = placed(
        jnp.broadcast_to(gain_ref[...].astype(F32), (ROWS, gain_ref.shape[-1]))
    ).astype(BF16)

    ids, gates = ids_ref[...], gates_ref[...]
    slots, seqs = out_ref.shape[0], ids.shape[1]
    experts = slots // CAP
    expert = me * experts + lax.broadcasted_iota(jnp.int32, (experts, seqs), 0)
    member, gate = jnp.zeros((experts, seqs), F32), jnp.zeros((experts, seqs), F32)
    for choice in range(ids.shape[0]):
        same = ids[choice : choice + 1] == expert
        member = jnp.where(same, 1.0, member)
        gate = jnp.where(same, gates[choice : choice + 1], gate)
    earlier = lax.broadcasted_iota(jnp.int32, (seqs, seqs), 0) < lax.broadcasted_iota(
        jnp.int32, (seqs, seqs), 1
    )
    rank = jnp.dot(
        member.astype(BF16), earlier.astype(F32).astype(BF16), preferred_element_type=F32
    )
    picks = [jnp.where(jnp.abs(rank - slot) < 0.5, member, 0.0) for slot in range(CAP)]
    pick_scr[...] = jnp.concatenate(picks, axis=0)
    slot_gates = [jnp.sum(pick * gate, axis=1, keepdims=True) for pick in picks]

    barrier = pltpu.get_barrier_semaphore()
    peers = [partner, across] + [device(zz, y, core) for zz in along]
    for peer in peers:
        pl.semaphore_signal(
            barrier, inc=1, device_id=peer, device_id_type=pl.DeviceIdType.MESH
        )
    pl.semaphore_wait(barrier, len(peers))

    pending = []

    def z_copies(source_of, target, send, recv):
        made = []
        for step, zz in enumerate(along):
            made.append(copy(source_of(zz), target, send.at[step], recv.at[step], device(zz, y, core)))
        return made

    def launch(made):
        for one in made:
            one.start()
            pending.append(one)
        return made

    gain_copy = launch(
        [copy(gainown, gainbuf, p_s.at[4], p_r.at[4], partner)]
    )
    q_along = [
        launch(z_copies(lambda zz: qown.at[k], qbuf.at[k, core, y, z], qz_s.at[k], qz_r.at[k]))
        for k in range(chunks)
    ]
    for k in range(chunks):
        qbuf[k, core, y, z] = qown[k]
    q_across, q_pair, o_pair, o_across, o_along = {}, {}, {}, {}, {}

    def gather_across(k):
        for one in q_along[k]:
            one.wait_recv()
        q_across[k] = launch(
            [copy(qbuf.at[k, core, y], qbuf.at[k, core, y], q_s.at[k, 0], q_r.at[k, 0], across)]
        )

    def gather_pair(k):
        q_across[k][0].wait_recv()
        q_pair[k] = launch(
            [copy(qbuf.at[k, core], qbuf.at[k, core], q_s.at[k, 1], q_r.at[k, 1], partner)]
        )

    ctx_local = cache.shape[2]
    count = CORES * LINKED_Y * zs
    position = me * ctx_local + lax.broadcasted_iota(jnp.int32, (2 * count, ctx_local), 1)

    def attend(k):
        q_pair[k][0].wait_recv()
        loads[k].wait()
        width = q_ref.shape[-1]
        rows = qbuf[k].reshape(count, ROWS, width).astype(F32)
        qrow[...] = jnp.swapaxes(rows, 0, 1).astype(BF16)

        scored = []
        for at in range(ROWS):
            row = qrow[at]
            latent = jnp.concatenate([row[:, :LAT], row[:, LAT : 2 * LAT]], axis=0)
            rotary = row[:, 2 * LAT :]
            rotary = jnp.concatenate([rotary[:, :ROPE], rotary[:, ROPE:]], axis=0)
            scores = jnp.dot(latent, cache[k * ROWS + at, :LAT], preferred_element_type=F32)
            scores = scores + jnp.dot(
                rotary, cache[k * ROWS + at, LAT:], preferred_element_type=F32
            )
            valid = position < ctx_ref[k * ROWS + at]
            scored.append(jnp.where(valid, scores * score_scale, masked_score))
        scores = jnp.stack(scored)
        top = jnp.max(scores, axis=2, keepdims=True)
        weights = jnp.where(scores > 0.5 * masked_score, jnp.exp(scores - top), 0.0)
        total = jnp.sum(weights, axis=2, keepdims=True)
        rounded = weights.astype(BF16)
        for at in range(ROWS):
            osc[at] = lax.dot_general(
                rounded[at],
                cache[k * ROWS + at, :LAT],
                (((1,), (1,)), ((), ())),
                preferred_element_type=F32,
            )
        columns = []
        for head in range(2):
            here = slice(head * count, (head + 1) * count)
            parts = split3(top[:, here]) + split3(total[:, here])
            columns += [(head * 6 + index, value) for index, value in enumerate(parts)]
        msc[...] = put_lanes((ROWS, count, LANES), columns)
        whole = jnp.swapaxes(osc[...], 0, 1).astype(BF16)
        shape = (CORES, LINKED_Y, zs, ROWS)
        s1[k, :, :, :, :, :LAT] = whole[:count].reshape(shape + (LAT,))
        s1[k, :, :, :, :, LAT : 2 * LAT] = whole[count:].reshape(shape + (LAT,))
        s1[k, :, :, :, :, 2 * LAT :] = (
            jnp.swapaxes(msc[...], 0, 1).astype(BF16).reshape(shape + (LANES,))
        )
        o_pair[k] = launch([copy(s1.at[k, 1 - core], r1.at[k], o_s.at[k, 0], o_r.at[k, 0], partner)])

    def merge_pair(k):
        o_pair[k][0].wait_recv()

        k1[k, 1 - y] = message(
            merge([s1[k, core, 1 - y].astype(F32), r1[k, 1 - y].astype(F32)])
        ).astype(BF16)
        o_across[k] = launch([copy(k1.at[k, 1 - y], r2.at[k], o_s.at[k, 1], o_r.at[k, 1], across)])

    def merge_across(k):
        o_across[k][0].wait_recv()

        k2[k] = message(
            merge([s1[k, core, y].astype(F32), r1[k, y].astype(F32), r2[k].astype(F32)])
        ).astype(BF16)
        o_along[k] = launch(
            [
                copy(k2.at[k, zz], r3.at[k, step], oz_s.at[k, step], oz_r.at[k, step], device(zz, y, core))
                for step, zz in enumerate(along)
            ]
        )

    def merge_along(k):
        for one in o_along[k]:
            one.wait_recv()
        blocks = [k2[k, z].astype(F32)] + [r3[k, step].astype(F32) for step in range(zs - 1)]
        for head, (out, _, total) in enumerate(merge(blocks)):
            merged[head, pl.ds(k * ROWS, ROWS), :] = out / total

    for t in range(chunks + 5):
        for stage, lag in (
            (gather_across, 0),
            (gather_pair, 1),
            (attend, 2),
            (merge_pair, 3),
            (merge_across, 4),
            (merge_along, 5),
        ):
            if 0 <= t - lag < chunks:
                stage(t - lag)

    values = []
    for head in range(2):
        own = merged[head]
        high = own.astype(BF16)
        low = (own - high.astype(F32)).astype(BF16)
        rows = up_ref[head * LAT : (head + 1) * LAT]
        values.append(
            jnp.dot(high, rows, preferred_element_type=F32)
            + jnp.dot(low, rows, preferred_element_type=F32)
        )
    value = jnp.concatenate(values, axis=1).astype(BF16)
    proj_load.wait()
    chip_cols = part.shape[-1]
    held = ps1.shape[-1]
    skip = chip_cols - held
    for zz in range(zs):
        for yy in range(LINKED_Y):
            start = (zz * LINKED_Y + yy) * chip_cols
            part[yy, zz] = jnp.dot(
                value, proj[:, start : start + chip_cols], preferred_element_type=F32
            )
    part[y, z] = part[y, z] + placed(resid_ref[...].astype(F32))
    own_cols = pl.ds(pl.multiple_of(core * skip, LANES), held)
    other_cols = pl.ds(pl.multiple_of((1 - core) * skip, LANES), held)
    ps1[...] = part[:, :, :, other_cols].astype(BF16)
    p_pair = launch([copy(ps1, pr1, p_s.at[0], p_r.at[0], partner)])
    p_pair[0].wait_recv()
    pk1[...] = (part[1 - y, :, :, own_cols] + pr1[1 - y].astype(F32)).astype(BF16)
    p_across = launch([copy(pk1, pr2, p_s.at[1], p_r.at[1], across)])
    p_across[0].wait_recv()
    kept = part[y, :, :, own_cols] + pr1[y].astype(F32) + pr2[...].astype(F32)
    part[y, :, :, own_cols] = kept
    pk2[...] = kept.astype(BF16)
    p_along = launch(
        [
            copy(pk2.at[zz], pr3.at[step], pz_s.at[0, step], pz_r.at[0, step], device(zz, y, core))
            for step, zz in enumerate(along)
        ]
    )
    gain_copy[0].wait_recv()
    for one in p_along:
        one.wait_recv()
    summed = part[y, z, :, own_cols]
    for step in range(zs - 1):
        summed = summed + pr3[step].astype(F32)
    gain = (gainown[...].astype(F32) + gainbuf[...].astype(F32))[:1]
    gain = jnp.where(core == 0, gain[:, :held], gain[:, skip:])
    scaled = summed * gain
    lane = lax.broadcasted_iota(jnp.int32, summed.shape, 1)
    first = jnp.where(core == 0, 0, 2 * held - chip_cols)
    square = jnp.sum(jnp.where(lane >= first, summed * summed, 0.0), axis=1, keepdims=True)
    largest = jnp.max(jnp.abs(scaled), axis=1, keepdims=True)
    columns = list(enumerate(split3(square) + split3(largest)))
    stats = put_lanes((summed.shape[0], LANES), columns)
    gbuf[core, y, z] = jnp.concatenate([scaled, stats], axis=1).astype(BF16)
    g_along = launch(
        [
            copy(
                gbuf.at[core, y, z],
                gbuf.at[core, y, z],
                pz_s.at[1, step],
                pz_r.at[1, step],
                device(zz, y, core),
            )
            for step, zz in enumerate(along)
        ]
    )
    for one in g_along:
        one.wait_recv()
    g_across = launch([copy(gbuf.at[core, y], gbuf.at[core, y], p_s.at[2], p_r.at[2], across)])
    g_across[0].wait_recv()
    g_pair = launch([copy(gbuf.at[core], gbuf.at[core], p_s.at[3], p_r.at[3], partner)])
    g_pair[0].wait_recv()

    stats = gbuf[:, :, :, :, held:].astype(F32).reshape(count, summed.shape[0], LANES)
    square = jnp.sum(take3(stats, 0), axis=0)
    largest = jnp.max(take3(stats, 3), axis=0)
    inverse = lax.rsqrt(square / (chip_cols * LINKED_Y * zs) + small_eps)
    peak = largest * inverse + small_eps
    factor = inverse / peak
    pick = pick_scr[...].astype(BF16)
    for zz in range(zs):
        for yy in range(LINKED_Y):
            start = (zz * LINKED_Y + yy) * chip_cols
            for cc in range(CORES):
                drop = cc * (2 * held - chip_cols)
                rows = gbuf[cc, yy, zz, :, drop:held].astype(F32) * factor
                at = start + cc * held
                out_ref[:, at : at + held - drop] = jnp.dot(
                    pick, rows.astype(BF16), preferred_element_type=F32
                ).astype(BF16)
    scales = jnp.dot(
        pick_scr[...],
        jnp.broadcast_to(peak, (peak.shape[0], LANES)),
        precision=lax.Precision.HIGHEST,
        preferred_element_type=F32,
    )
    wide = jnp.broadcast_to(jnp.concatenate(slot_gates, axis=0), (slots, LANES))
    tail = jnp.zeros((LANES - 2 * slots, LANES), F32)
    flat = jnp.transpose(jnp.concatenate([scales, wide, tail], axis=0))
    scale_ref[...] = flat[:ROWS]
    for one in pending:
        one.wait_send()


def fused_device(
    queries,
    latent_cache,
    context_lengths,
    value_up,
    out_proj,
    residual,
    norm_gain,
    expert_ids,
    gate_weights,
):
    kv_count = lax.axis_size("kv")
    zs = kv_count // (CORES * LINKED_Y)
    seq_count = queries.shape[0]
    chunks = seq_count // ROWS
    ctx_local = latent_cache.shape[1]
    width = queries.shape[1]
    cols = residual.shape[1]
    chip_cols = cols * CORES
    held = -(-cols // LANES) * LANES
    experts_local = EXPERTS // kv_count
    slot_count = experts_local * CAP
    vmem = pl.BlockSpec(memory_space=pltpu.VMEM)
    smem = pl.BlockSpec(memory_space=pltpu.SMEM)
    anywhere = pl.BlockSpec(memory_space=pl.ANY)
    dma = pltpu.SemaphoreType.DMA
    full = (LINKED_Y, zs)
    dispatched, scale = pl.pallas_call(
        functools.partial(step_kernel, zs, chunks),
        out_shape=(
            jax.ShapeDtypeStruct((slot_count, chip_cols * LINKED_Y * zs), BF16),
            jax.ShapeDtypeStruct((ROWS, LANES), F32),
        ),
        in_specs=[vmem, anywhere, smem, vmem, anywhere, vmem, vmem, vmem, vmem],
        out_specs=(vmem, vmem),
        scratch_shapes=[
            pltpu.VMEM((chunks, ROWS, width), BF16),
            pltpu.VMEM((ROWS, chip_cols), BF16),
            pltpu.VMEM((slot_count, seq_count), F32),
            pltpu.VMEM((seq_count, LAT + ROPE, ctx_local), BF16),
            pltpu.VMEM(out_proj.shape, BF16),
            pltpu.VMEM((chunks, CORES) + full + (ROWS, width), BF16),
            pltpu.VMEM((ROWS, kv_count, width), BF16),
            pltpu.VMEM((ROWS, H, LAT), F32),
            pltpu.VMEM((ROWS, kv_count, LANES), F32),
            pltpu.VMEM((chunks, CORES) + full + (ROWS, width), BF16),
            pltpu.VMEM((chunks,) + full + (ROWS, width), BF16),
            pltpu.VMEM((chunks,) + full + (ROWS, width), BF16),
            pltpu.VMEM((chunks, zs, ROWS, width), BF16),
            pltpu.VMEM((chunks, zs, ROWS, width), BF16),
            pltpu.VMEM((chunks, zs - 1, ROWS, width), BF16),
            pltpu.VMEM((H // kv_count, seq_count, LAT), F32),
            pltpu.VMEM(full + (seq_count, chip_cols), F32),
            pltpu.VMEM(full + (seq_count, held), BF16),
            pltpu.VMEM(full + (seq_count, held), BF16),
            pltpu.VMEM((zs, seq_count, held), BF16),
            pltpu.VMEM((zs, seq_count, held), BF16),
            pltpu.VMEM((zs, seq_count, held), BF16),
            pltpu.VMEM((zs - 1, seq_count, held), BF16),
            pltpu.VMEM((CORES,) + full + (seq_count, held + LANES), BF16),
            pltpu.VMEM((ROWS, chip_cols), BF16),
            dma((chunks,)),
            dma,
            dma((chunks, zs - 1)),
            dma((chunks, zs - 1)),
            dma((chunks, 2)),
            dma((chunks, 2)),
            dma((chunks, zs - 1)),
            dma((chunks, zs - 1)),
            dma((chunks, 2)),
            dma((chunks, 2)),
            dma((2, zs - 1)),
            dma((2, zs - 1)),
            dma((5,)),
            dma((5,)),
        ],
        compiler_params=pltpu.CompilerParams(
            collective_id=0, has_side_effects=True, vmem_limit_bytes=60 * 1024 * 1024
        ),
    )(
        queries.reshape(chunks, ROWS, width),
        jnp.swapaxes(latent_cache, 1, 2),
        context_lengths,
        value_up,
        out_proj,
        residual,
        norm_gain.reshape(1, -1),
        expert_ids.T,
        gate_weights.T,
    )
    split = jnp.swapaxes(dispatched.reshape(CAP, experts_local, -1), 0, 1)
    scale = scale[0].reshape(-1, CAP, experts_local)
    return split, scale[0].T, scale[1].T


def per_device(*arrays):
    queries, residual = arrays[0], arrays[5]
    kv_count = lax.axis_size("kv")
    pairs = H == 2 * kv_count and EXPERTS * CAP * 2 <= kv_count * LANES and 2 * ROPE == LANES and kv_count % (CORES * LINKED_Y) == 0
    aligned = queries.shape[0] % ROWS == 0 and residual.shape[1] * CORES % LANES == 0
    if pairs and aligned:
        return fused_device(*arrays)
    return general_device(*arrays)


def solution(mesh):
    in_specs = (
        P("groups", "kv"),
        P("groups", "kv", None),
        P("groups"),
        P("kv", None),
        P("kv", None),
        P("groups", "kv"),
        P("kv"),
        P("groups", None),
        P("groups", None),
    )
    out_specs = (
        P(("groups", "kv"), None, None),
        P(("groups", "kv"), None),
        P(("groups", "kv"), None),
    )
    return jax.shard_map(
        per_device, mesh=mesh, in_specs=in_specs, out_specs=out_specs, check_vma=False
    )
```

```python
import functools

import jax
import jax.numpy as jnp
from jax import lax
from jax.experimental import pallas as pl
from jax.experimental.pallas import tpu as pltpu
from jax.sharding import PartitionSpec as P

H = 32
LAT = 512
ROPE = 64
VD = 128
D = 7168
EXPERTS = 256
TOPK = 8
CAP = 2


score_scale = 192.0 ** (-0.5)
masked_score = -1e30
small_eps = 1e-06


def from_partner(value, axis, bit):
    mask = 2**bit
    pairs = [(source, source ^ mask) for source in range(lax.axis_size(axis))]
    return lax.ppermute(value, axis, pairs)


def slot_targets(expert_ids):
    flat_ids = expert_ids.reshape(-1)
    order_index = jnp.arange(flat_ids.shape[0], dtype=jnp.int32)
    same_before = (flat_ids[:, None] == flat_ids[None, :]) & (
        order_index[None, :] < order_index[:, None]
    )
    rank_within = jnp.sum(same_before.astype(jnp.int32), axis=1)
    return flat_ids * CAP + rank_within


def slot_match(targets, first_slot, slot_count):
    slot_index = first_slot + jnp.arange(slot_count, dtype=jnp.int32)
    return (slot_index[:, None] == targets[None, :]).astype(jnp.float32)


def token_picker(matches, seq_count):
    return jnp.sum(matches.reshape(matches.shape[0], seq_count, TOPK), axis=2)


def general_device(
    queries,
    latent_cache,
    context_lengths,
    value_up,
    out_proj,
    residual,
    norm_gain,
    expert_ids,
    gate_weights,
):
    kv_count = lax.axis_size("kv")
    shard_index = lax.axis_index("kv")
    seq_count = queries.shape[0]
    query_rows = lax.all_gather(queries, "kv", axis=1, tiled=True).reshape(seq_count, H, LAT + ROPE)
    ctx_local = latent_cache.shape[1]
    scores = (
        jnp.einsum("shq,scq->shc", query_rows, latent_cache, preferred_element_type=jnp.float32)
        * score_scale
    )
    position = shard_index * ctx_local + jnp.arange(ctx_local, dtype=jnp.int32)
    valid_mask = (position[None, :] < context_lengths[:, None])[:, None, :]
    scores = jnp.where(valid_mask, scores, masked_score)
    local_max = jnp.max(scores, axis=2)
    weights = jnp.where(valid_mask, jnp.exp(scores - local_max[:, :, None]), 0.0)
    local_total = jnp.sum(weights, axis=2)
    local_out = jnp.einsum(
        "shc,scl->shl",
        weights.astype(jnp.bfloat16),
        latent_cache[:, :, :LAT],
        preferred_element_type=jnp.float32,
    )
    out_rows = out_proj.shape[0]
    col_count = H * LAT // kv_count
    segment = min(col_count, LAT)
    head_count = col_count // segment
    head_start = shard_index * col_count // LAT
    global_max = lax.pmax(local_max, "kv")
    scaling = jnp.exp(local_max - global_max)
    weight_total = lax.psum(local_total * scaling, "kv")
    scaled = (local_out * scaling[:, :, None]).reshape(seq_count, H * LAT)
    merged_sum = lax.psum_scatter(scaled, "kv", scatter_dimension=1, tiled=True).reshape(
        seq_count, head_count, segment
    )
    own_total = lax.dynamic_slice_in_dim(weight_total, head_start, head_count, 1)
    merged = merged_sum / own_total[:, :, None]
    projector = value_up.reshape(head_count, segment, VD).astype(jnp.float32)
    value_part = jnp.einsum("shl,hlv->shv", merged, projector, precision=lax.Precision.HIGHEST)
    holders = kv_count // H if kv_count > H else 1
    for bit in range(holders.bit_length() - 1):
        value_part = value_part + from_partner(value_part, "kv", bit)
    value_rows = value_part.astype(jnp.bfloat16).reshape(seq_count, head_count * VD)
    if holders > 1:
        value_rows = lax.dynamic_slice_in_dim(
            value_rows, shard_index % holders * out_rows, out_rows, 1
        )
    partial_out = jnp.dot(value_rows, out_proj, preferred_element_type=jnp.float32)
    experts_local = EXPERTS // kv_count
    slot_count = experts_local * CAP
    targets = slot_targets(expert_ids)
    own_match = slot_match(targets, shard_index * slot_count, slot_count)
    own_pick = token_picker(own_match, seq_count)
    slot_gate = jnp.dot(own_match, gate_weights.reshape(-1), precision=lax.Precision.HIGHEST)
    attn_rows = lax.psum(partial_out, "kv")
    resid_rows, gain_cols = (
        lax.all_gather(residual, "kv", axis=1, tiled=True),
        lax.all_gather(norm_gain, "kv", axis=0, tiled=True),
    )
    summed = attn_rows + resid_rows.astype(jnp.float32)
    inverse_rms = lax.rsqrt(jnp.mean(summed * summed, axis=1) + small_eps)
    normed = summed * inverse_rms[:, None] * gain_cols.astype(jnp.float32)
    peak_abs = jnp.max(jnp.abs(normed), axis=1) + small_eps
    coded_rows = (normed / peak_abs[:, None]).astype(jnp.bfloat16)
    dispatched = jnp.dot(
        own_pick.astype(jnp.bfloat16), coded_rows, preferred_element_type=jnp.float32
    ).astype(jnp.bfloat16)
    slot_scale = jnp.dot(own_pick, peak_abs, precision=lax.Precision.HIGHEST)
    return (
        dispatched.reshape(experts_local, CAP, D),
        slot_scale.reshape(experts_local, CAP),
        slot_gate.reshape(experts_local, CAP),
    )


CORES = 2
LINKED_Y = 2
LANES = 128
ROWS = 8
GROUP = 2
F32 = jnp.float32
BF16 = jnp.bfloat16


def split3(value):
    first = value.astype(BF16).astype(F32)
    rest = value - first
    second = rest.astype(BF16).astype(F32)
    return first, second, rest - second


def put_lanes(shape, columns):
    lane = lax.broadcasted_iota(jnp.int32, shape, len(shape) - 1)
    tile = jnp.zeros(shape, F32)
    for index, column in columns:
        tile = jnp.where(lane == index, column, tile)
    return tile


def take3(tile, start):
    return (
        tile[..., start : start + 1]
        + tile[..., start + 1 : start + 2]
        + tile[..., start + 2 : start + 3]
    )


def merge(blocks):
    heads = (blocks[0].shape[-1] - LANES) // LAT
    outs, columns = [], []
    for head in range(heads):
        stats = [block[..., heads * LAT :] for block in blocks]
        maxes = [take3(stat, head * 6) for stat in stats]
        totals = [take3(stat, head * 6 + 3) for stat in stats]
        top = maxes[0]
        for other in maxes[1:]:
            top = jnp.maximum(top, other)
        total, out = 0.0, 0.0
        for block, own_max, own_total in zip(blocks, maxes, totals):
            factor = jnp.exp(own_max - top)
            total = total + factor * own_total
            out = out + factor * block[..., head * LAT : (head + 1) * LAT]
        outs.append((out, top, total))
    return outs


def message(outs):
    columns = []
    for head, (out, top, total) in enumerate(outs):
        for index, part in enumerate(split3(top) + split3(total)):
            columns.append((head * 6 + index, part))
    shape = outs[0][0].shape[:-1] + (LANES,)
    return jnp.concatenate([out for out, _, _ in outs] + [put_lanes(shape, columns)], axis=-1)


def step_kernel(
    zs,
    chunks,
    q_ref,
    cache_hbm,
    ctx_ref,
    up_ref,
    proj_hbm,
    resid_ref,
    gain_ref,
    ids_ref,
    gates_ref,
    out_ref,
    scale_ref,
    qown,
    pick_scr,
    cache,
    proj,
    qbuf,
    qrow,
    osc,
    msc,
    s1,
    r1,
    k1,
    r2,
    k2,
    r3,
    merged,
    mine,
    ps1,
    pr1,
    pk1,
    pr2,
    pk2,
    pr3,
    gbuf,
    codes,
    peaks,
    load_sem,
    proj_sem,
    qz_s,
    qz_r,
    q_s,
    q_r,
    oz_s,
    oz_r,
    o_s,
    o_r,
    pz_s,
    pz_r,
    p_s,
    p_r,
):
    me = lax.axis_index("kv")
    core = lax.rem(me, CORES)
    y = lax.rem(me // CORES, LINKED_Y)
    z = me // (CORES * LINKED_Y)

    def device(zz, yy, cc):
        return {"kv": (zz * LINKED_Y + yy) * CORES + cc}

    partner = device(z, y, 1 - core)
    across = device(z, 1 - y, core)
    along = [lax.rem(z + step, zs) for step in range(1, zs)]
    back = [lax.rem(z + zs - step, zs) for step in range(1, zs)]

    def copy(source, target, send, recv, where):
        return pltpu.make_async_remote_copy(
            src_ref=source,
            dst_ref=target,
            send_sem=send,
            recv_sem=recv,
            device_id=where,
            device_id_type=pl.DeviceIdType.MESH,
        )

    loads = [
        pltpu.make_async_copy(
            cache_hbm.at[pl.ds(k * ROWS, ROWS)], cache.at[pl.ds(k * ROWS, ROWS)], load_sem.at[k]
        )
        for k in range(chunks)
    ]
    for load in loads:
        load.start()
    proj_load = pltpu.make_async_copy(proj_hbm, proj, proj_sem)
    proj_load.start()

    raw = q_ref[...].astype(F32)
    key = LAT + ROPE
    qown[...] = jnp.concatenate(
        [raw[..., :LAT], raw[..., key : key + LAT], raw[..., LAT:key], raw[..., key + LAT :]],
        axis=-1,
    ).astype(BF16)

    ids, gates = ids_ref[...], gates_ref[...]
    slots, seqs = out_ref.shape[0], ids.shape[1]
    experts = slots // CAP
    expert = me * experts + lax.broadcasted_iota(jnp.int32, (experts, seqs), 0)
    member, gate = jnp.zeros((experts, seqs), F32), jnp.zeros((experts, seqs), F32)
    for choice in range(ids.shape[0]):
        same = ids[choice : choice + 1] == expert
        member = jnp.where(same, 1.0, member)
        gate = jnp.where(same, gates[choice : choice + 1], gate)
    earlier = lax.broadcasted_iota(jnp.int32, (seqs, seqs), 0) < lax.broadcasted_iota(
        jnp.int32, (seqs, seqs), 1
    )
    rank = jnp.dot(
        member.astype(BF16), earlier.astype(F32).astype(BF16), preferred_element_type=F32
    )
    picks = [jnp.where(jnp.abs(rank - slot) < 0.5, member, 0.0) for slot in range(CAP)]
    pick_scr[...] = jnp.concatenate(picks, axis=0)
    slot_gates = [jnp.sum(pick * gate, axis=1, keepdims=True) for pick in picks]

    barrier = pltpu.get_barrier_semaphore()
    peers = [partner, across] + [device(zz, y, core) for zz in along]
    for peer in peers:
        pl.semaphore_signal(
            barrier, inc=1, device_id=peer, device_id_type=pl.DeviceIdType.MESH
        )
    pl.semaphore_wait(barrier, len(peers))

    pending = []

    def z_copies(source_of, target, send, recv):
        made = []
        for step, zz in enumerate(along):
            made.append(copy(source_of(zz), target, send.at[step], recv.at[step], device(zz, y, core)))
        return made

    def launch(made):
        for one in made:
            one.start()
            pending.append(one)
        return made

    q_along = [
        launch(z_copies(lambda zz: qown.at[k], qbuf.at[k, core, y, z], qz_s.at[k], qz_r.at[k]))
        for k in range(chunks)
    ]
    for k in range(chunks):
        qbuf[k, core, y, z] = qown[k]
    q_across, q_pair, o_pair, o_across, o_along = {}, {}, {}, {}, {}

    def gather_across(k):
        for one in q_along[k]:
            one.wait_recv()
        q_across[k] = launch(
            [copy(qbuf.at[k, core, y], qbuf.at[k, core, y], q_s.at[k, 0], q_r.at[k, 0], across)]
        )

    def gather_pair(k):
        q_across[k][0].wait_recv()
        q_pair[k] = launch(
            [copy(qbuf.at[k, core], qbuf.at[k, core], q_s.at[k, 1], q_r.at[k, 1], partner)]
        )

    ctx_local = cache.shape[2]
    count = CORES * LINKED_Y * zs
    position = me * ctx_local + lax.broadcasted_iota(jnp.int32, (2 * count, ctx_local), 1)

    def attend(k):
        q_pair[k][0].wait_recv()
        loads[k].wait()
        width = q_ref.shape[-1]
        rows = qbuf[k].reshape(count, ROWS, width).astype(F32)
        qrow[...] = jnp.swapaxes(rows, 0, 1).astype(BF16)

        scored = []
        for at in range(ROWS):
            row = qrow[at]
            latent = jnp.concatenate([row[:, :LAT], row[:, LAT : 2 * LAT]], axis=0)
            rotary = row[:, 2 * LAT :]
            rotary = jnp.concatenate([rotary[:, :ROPE], rotary[:, ROPE:]], axis=0)
            scores = jnp.dot(latent, cache[k * ROWS + at, :LAT], preferred_element_type=F32)
            scores = scores + jnp.dot(
                rotary, cache[k * ROWS + at, LAT:], preferred_element_type=F32
            )
            valid = position < ctx_ref[k * ROWS + at]
            scored.append(jnp.where(valid, scores * score_scale, masked_score))
        scores = jnp.stack(scored)
        top = jnp.max(scores, axis=2, keepdims=True)
        weights = jnp.where(scores > 0.5 * masked_score, jnp.exp(scores - top), 0.0)
        total = jnp.sum(weights, axis=2, keepdims=True)
        rounded = weights.astype(BF16)
        for at in range(ROWS):
            osc[at] = lax.dot_general(
                rounded[at],
                cache[k * ROWS + at, :LAT],
                (((1,), (1,)), ((), ())),
                preferred_element_type=F32,
            )
        columns = []
        for head in range(2):
            here = slice(head * count, (head + 1) * count)
            parts = split3(top[:, here]) + split3(total[:, here])
            columns += [(head * 6 + index, value) for index, value in enumerate(parts)]
        msc[...] = put_lanes((ROWS, count, LANES), columns)
        whole = jnp.swapaxes(osc[...], 0, 1).astype(BF16)
        shape = (CORES, LINKED_Y, zs, ROWS)
        s1[k, :, :, :, :, :LAT] = whole[:count].reshape(shape + (LAT,))
        s1[k, :, :, :, :, LAT : 2 * LAT] = whole[count:].reshape(shape + (LAT,))
        s1[k, :, :, :, :, 2 * LAT :] = (
            jnp.swapaxes(msc[...], 0, 1).astype(BF16).reshape(shape + (LANES,))
        )
        o_pair[k] = launch([copy(s1.at[k, 1 - core], r1.at[k], o_s.at[k, 0], o_r.at[k, 0], partner)])

    def merge_pair(k):
        o_pair[k][0].wait_recv()

        k1[k, 1 - y] = message(
            merge([s1[k, core, 1 - y].astype(F32), r1[k, 1 - y].astype(F32)])
        ).astype(BF16)
        o_across[k] = launch([copy(k1.at[k, 1 - y], r2.at[k], o_s.at[k, 1], o_r.at[k, 1], across)])

    def merge_across(k):
        o_across[k][0].wait_recv()

        k2[k] = message(
            merge([s1[k, core, y].astype(F32), r1[k, y].astype(F32), r2[k].astype(F32)])
        ).astype(BF16)
        o_along[k] = launch(
            [
                copy(k2.at[k, zz], r3.at[k, step], oz_s.at[k, step], oz_r.at[k, step], device(zz, y, core))
                for step, zz in enumerate(along)
            ]
        )

    def merge_along(k):
        for one in o_along[k]:
            one.wait_recv()
        blocks = [k2[k, z].astype(F32)] + [r3[k, step].astype(F32) for step in range(zs - 1)]
        for head, (out, _, total) in enumerate(merge(blocks)):
            merged[head, pl.ds(k * ROWS, ROWS), :] = out / total

    cols = resid_ref.shape[-1]
    chip_cols = cols * CORES
    p_pair, p_across, p_along, g_along, g_across, g_pair = {}, {}, {}, {}, {}, {}

    def span(g):
        first = g * GROUP
        return first, min(GROUP, chunks - first)

    def project(g):
        first, size = span(g)
        values = []
        for head in range(2):
            own = merged[head, pl.ds(first * ROWS, size * ROWS), :]
            high = own.astype(BF16)
            low = (own - high.astype(F32)).astype(BF16)
            rows = up_ref[head * LAT : (head + 1) * LAT]
            values.append(
                jnp.dot(high, rows, preferred_element_type=F32)
                + jnp.dot(low, rows, preferred_element_type=F32)
            )
        value = jnp.concatenate(values, axis=1).astype(BF16)
        if g == 0:
            proj_load.wait()
        here = pl.ds(first, size)
        for zz in range(zs):
            for yy in range(LINKED_Y):
                start = (zz * LINKED_Y + yy) * chip_cols
                both = jnp.dot(
                    value, proj[:, start : start + chip_cols], preferred_element_type=F32
                ).reshape(size, ROWS, chip_cols)
                low, high = both[..., :cols], both[..., cols:]
                mine[here, yy, zz] = jnp.where(core == 0, low, high)
                ps1[here, yy, zz] = jnp.where(core == 0, high, low).astype(BF16)
        p_pair[g] = launch([copy(ps1.at[here], pr1.at[here], p_s.at[g, 0], p_r.at[g, 0], partner)])

    def sum_pair(g):
        here = pl.ds(*span(g))
        p_pair[g][0].wait_recv()
        pk1[here] = (mine[here, 1 - y] + pr1[here, 1 - y].astype(F32)).astype(BF16)
        p_across[g] = launch([copy(pk1.at[here], pr2.at[here], p_s.at[g, 1], p_r.at[g, 1], across)])

    def sum_across(g):
        here = pl.ds(*span(g))
        p_across[g][0].wait_recv()
        kept = mine[here, y] + pr1[here, y].astype(F32) + pr2[here].astype(F32)
        mine[here, y] = kept
        pk2[here] = kept.astype(BF16)
        p_along[g] = launch(
            [
                copy(
                    pk2.at[here, zz],
                    pr3.at[step, here],
                    pz_s.at[g, 0, step],
                    pz_r.at[g, 0, step],
                    device(zz, y, core),
                )
                for step, zz in enumerate(along)
            ]
        )

    def sum_along(g):
        here = pl.ds(*span(g))
        for one in p_along[g]:
            one.wait_recv()
        summed = mine[here, y, z] + resid_ref[here].astype(F32)
        for step in range(zs - 1):
            summed = summed + pr3[step, here].astype(F32)
        scaled = summed * gain_ref[...].astype(F32)
        square = jnp.sum(summed * summed, axis=-1, keepdims=True)
        largest = jnp.max(jnp.abs(scaled), axis=-1, keepdims=True)
        shape = summed.shape[:-1] + (gbuf.shape[-1] - cols,)
        stats = put_lanes(shape, list(enumerate(split3(square) + split3(largest))))
        gbuf[here, core, y, z] = jnp.concatenate([scaled, stats], axis=-1).astype(BF16)
        block = gbuf.at[here, core, y, z]
        g_along[g] = launch(
            [
                copy(block, block, pz_s.at[g, 1, step], pz_r.at[g, 1, step], device(zz, y, core))
                for step, zz in enumerate(along)
            ]
        )

    def spread_across(g):
        here = pl.ds(*span(g))
        for one in g_along[g]:
            one.wait_recv()
        block = gbuf.at[here, core, y]
        g_across[g] = launch([copy(block, block, p_s.at[g, 2], p_r.at[g, 2], across)])

    def spread_pair(g):
        here = pl.ds(*span(g))
        g_across[g][0].wait_recv()
        block = gbuf.at[here, core]
        g_pair[g] = launch([copy(block, block, p_s.at[g, 3], p_r.at[g, 3], partner)])

    def finish(g):
        first, size = span(g)
        g_pair[g][0].wait_recv()
        for k in range(first, first + size):
            here = pl.ds(k * ROWS, ROWS)
            stats = gbuf[k, :, :, :, :, cols:].astype(F32).reshape(count, ROWS, -1)
            square = jnp.sum(take3(stats, 0), axis=0)
            largest = jnp.max(take3(stats, 3), axis=0)
            inverse = lax.rsqrt(square / (chip_cols * LINKED_Y * zs) + small_eps)
            peak = largest * inverse + small_eps
            factor = inverse / peak
            peaks[here] = jnp.broadcast_to(peak, (ROWS, LANES))
            for zz in range(zs):
                for yy in range(LINKED_Y):
                    start = (zz * LINKED_Y + yy) * chip_cols
                    rows = [gbuf[k, cc, yy, zz, :, :cols].astype(F32) for cc in range(CORES)]
                    codes[here, start : start + chip_cols] = (
                        jnp.concatenate(rows, axis=1) * factor
                    ).astype(BF16)

    chunk_stages = (gather_across, gather_pair, attend, merge_pair, merge_across, merge_along)
    group_stages = (
        project,
        sum_pair,
        sum_across,
        sum_along,
        spread_across,
        spread_pair,
        finish,
    )
    groups = -(-chunks // GROUP)
    for t in range(chunks + len(chunk_stages) + len(group_stages)):
        for lag, stage in enumerate(chunk_stages):
            if 0 <= t - lag < chunks:
                stage(t - lag)
        for lag, stage in enumerate(group_stages):
            for g in range(groups):
                if sum(span(g)) - 1 + len(chunk_stages) - 1 + lag == t:
                    stage(g)

    pick = pick_scr[...].astype(BF16)
    for start in range(0, codes.shape[1], chip_cols):
        out_ref[:, start : start + chip_cols] = jnp.dot(
            pick, codes[:, start : start + chip_cols], preferred_element_type=F32
        ).astype(BF16)
    scales = jnp.dot(
        pick_scr[...],
        peaks[...],
        precision=lax.Precision.HIGHEST,
        preferred_element_type=F32,
    )
    wide = jnp.broadcast_to(jnp.concatenate(slot_gates, axis=0), (slots, LANES))
    tail = jnp.zeros((LANES - 2 * slots, LANES), F32)
    flat = jnp.transpose(jnp.concatenate([scales, wide, tail], axis=0))
    scale_ref[...] = flat[:ROWS]
    for one in pending:
        one.wait_send()


def fused_device(
    queries,
    latent_cache,
    context_lengths,
    value_up,
    out_proj,
    residual,
    norm_gain,
    expert_ids,
    gate_weights,
):
    kv_count = lax.axis_size("kv")
    zs = kv_count // (CORES * LINKED_Y)
    seq_count = queries.shape[0]
    chunks = seq_count // ROWS
    ctx_local = latent_cache.shape[1]
    width = queries.shape[1]
    cols = residual.shape[1]
    chip_cols = cols * CORES
    held = -(-(cols + 6) // LANES) * LANES
    groups = -(-chunks // GROUP)
    experts_local = EXPERTS // kv_count
    slot_count = experts_local * CAP
    vmem = pl.BlockSpec(memory_space=pltpu.VMEM)
    smem = pl.BlockSpec(memory_space=pltpu.SMEM)
    anywhere = pl.BlockSpec(memory_space=pl.ANY)
    dma = pltpu.SemaphoreType.DMA
    full = (LINKED_Y, zs)
    dispatched, scale = pl.pallas_call(
        functools.partial(step_kernel, zs, chunks),
        out_shape=(
            jax.ShapeDtypeStruct((slot_count, chip_cols * LINKED_Y * zs), BF16),
            jax.ShapeDtypeStruct((ROWS, LANES), F32),
        ),
        in_specs=[vmem, anywhere, smem, vmem, anywhere, vmem, vmem, vmem, vmem],
        out_specs=(vmem, vmem),
        scratch_shapes=[
            pltpu.VMEM((chunks, ROWS, width), BF16),
            pltpu.VMEM((slot_count, seq_count), F32),
            pltpu.VMEM((seq_count, LAT + ROPE, ctx_local), BF16),
            pltpu.VMEM(out_proj.shape, BF16),
            pltpu.VMEM((chunks, CORES) + full + (ROWS, width), BF16),
            pltpu.VMEM((ROWS, kv_count, width), BF16),
            pltpu.VMEM((ROWS, H, LAT), F32),
            pltpu.VMEM((ROWS, kv_count, LANES), F32),
            pltpu.VMEM((chunks, CORES) + full + (ROWS, width), BF16),
            pltpu.VMEM((chunks,) + full + (ROWS, width), BF16),
            pltpu.VMEM((chunks,) + full + (ROWS, width), BF16),
            pltpu.VMEM((chunks, zs, ROWS, width), BF16),
            pltpu.VMEM((chunks, zs, ROWS, width), BF16),
            pltpu.VMEM((chunks, zs - 1, ROWS, width), BF16),
            pltpu.VMEM((H // kv_count, seq_count, LAT), F32),
            pltpu.VMEM((chunks,) + full + (ROWS, cols), F32),
            pltpu.VMEM((chunks,) + full + (ROWS, cols), BF16),
            pltpu.VMEM((chunks,) + full + (ROWS, cols), BF16),
            pltpu.VMEM((chunks, zs, ROWS, cols), BF16),
            pltpu.VMEM((chunks, zs, ROWS, cols), BF16),
            pltpu.VMEM((chunks, zs, ROWS, cols), BF16),
            pltpu.VMEM((zs - 1, chunks, ROWS, cols), BF16),
            pltpu.VMEM((chunks, CORES) + full + (ROWS, held), BF16),
            pltpu.VMEM((seq_count, chip_cols * LINKED_Y * zs), BF16),
            pltpu.VMEM((seq_count, LANES), F32),
            dma((chunks,)),
            dma,
            dma((chunks, zs - 1)),
            dma((chunks, zs - 1)),
            dma((chunks, 2)),
            dma((chunks, 2)),
            dma((chunks, zs - 1)),
            dma((chunks, zs - 1)),
            dma((chunks, 2)),
            dma((chunks, 2)),
            dma((groups, 2, zs - 1)),
            dma((groups, 2, zs - 1)),
            dma((groups, 4)),
            dma((groups, 4)),
        ],
        compiler_params=pltpu.CompilerParams(
            collective_id=0, has_side_effects=True, vmem_limit_bytes=60 * 1024 * 1024
        ),
    )(
        queries.reshape(chunks, ROWS, width),
        jnp.swapaxes(latent_cache, 1, 2),
        context_lengths,
        value_up,
        out_proj,
        residual.reshape(chunks, ROWS, cols),
        norm_gain.reshape(1, -1),
        expert_ids.T,
        gate_weights.T,
    )
    split = jnp.swapaxes(dispatched.reshape(CAP, experts_local, -1), 0, 1)
    scale = scale[0].reshape(-1, CAP, experts_local)
    return split, scale[0].T, scale[1].T


def per_device(*arrays):
    queries, residual = arrays[0], arrays[5]
    kv_count = lax.axis_size("kv")
    pairs = H == 2 * kv_count and EXPERTS * CAP * 2 <= kv_count * LANES and 2 * ROPE == LANES and kv_count % (CORES * LINKED_Y) == 0
    aligned = queries.shape[0] % ROWS == 0 and residual.shape[1] * CORES % LANES == 0
    if pairs and aligned:
        return fused_device(*arrays)
    return general_device(*arrays)


def solution(mesh):
    in_specs = (
        P("groups", "kv"),
        P("groups", "kv", None),
        P("groups"),
        P("kv", None),
        P("kv", None),
        P("groups", "kv"),
        P("kv"),
        P("groups", None),
        P("groups", None),
    )
    out_specs = (
        P(("groups", "kv"), None, None),
        P(("groups", "kv"), None),
        P(("groups", "kv"), None),
    )
    return jax.shard_map(
        per_device, mesh=mesh, in_specs=in_specs, out_specs=out_specs, check_vma=False
    )
```

```python
import functools

import jax
import jax.numpy as jnp
from jax import lax
from jax.experimental import pallas as pl
from jax.experimental.pallas import tpu as pltpu
from jax.sharding import PartitionSpec as P

H = 32
LAT = 512
ROPE = 64
VD = 128
D = 7168
EXPERTS = 256
TOPK = 8
CAP = 2


score_scale = 192.0 ** (-0.5)
masked_score = -1e30
small_eps = 1e-06


def from_partner(value, axis, bit):
    mask = 2**bit
    pairs = [(source, source ^ mask) for source in range(lax.axis_size(axis))]
    return lax.ppermute(value, axis, pairs)


def slot_targets(expert_ids):
    flat_ids = expert_ids.reshape(-1)
    order_index = jnp.arange(flat_ids.shape[0], dtype=jnp.int32)
    same_before = (flat_ids[:, None] == flat_ids[None, :]) & (
        order_index[None, :] < order_index[:, None]
    )
    rank_within = jnp.sum(same_before.astype(jnp.int32), axis=1)
    return flat_ids * CAP + rank_within


def slot_match(targets, first_slot, slot_count):
    slot_index = first_slot + jnp.arange(slot_count, dtype=jnp.int32)
    return (slot_index[:, None] == targets[None, :]).astype(jnp.float32)


def token_picker(matches, seq_count):
    return jnp.sum(matches.reshape(matches.shape[0], seq_count, TOPK), axis=2)


def general_device(
    queries,
    latent_cache,
    context_lengths,
    value_up,
    out_proj,
    residual,
    norm_gain,
    expert_ids,
    gate_weights,
):
    kv_count = lax.axis_size("kv")
    shard_index = lax.axis_index("kv")
    seq_count = queries.shape[0]
    query_rows = lax.all_gather(queries, "kv", axis=1, tiled=True).reshape(seq_count, H, LAT + ROPE)
    ctx_local = latent_cache.shape[1]
    scores = (
        jnp.einsum("shq,scq->shc", query_rows, latent_cache, preferred_element_type=jnp.float32)
        * score_scale
    )
    position = shard_index * ctx_local + jnp.arange(ctx_local, dtype=jnp.int32)
    valid_mask = (position[None, :] < context_lengths[:, None])[:, None, :]
    scores = jnp.where(valid_mask, scores, masked_score)
    local_max = jnp.max(scores, axis=2)
    weights = jnp.where(valid_mask, jnp.exp(scores - local_max[:, :, None]), 0.0)
    local_total = jnp.sum(weights, axis=2)
    local_out = jnp.einsum(
        "shc,scl->shl",
        weights.astype(jnp.bfloat16),
        latent_cache[:, :, :LAT],
        preferred_element_type=jnp.float32,
    )
    out_rows = out_proj.shape[0]
    col_count = H * LAT // kv_count
    segment = min(col_count, LAT)
    head_count = col_count // segment
    head_start = shard_index * col_count // LAT
    global_max = lax.pmax(local_max, "kv")
    scaling = jnp.exp(local_max - global_max)
    weight_total = lax.psum(local_total * scaling, "kv")
    scaled = (local_out * scaling[:, :, None]).reshape(seq_count, H * LAT)
    merged_sum = lax.psum_scatter(scaled, "kv", scatter_dimension=1, tiled=True).reshape(
        seq_count, head_count, segment
    )
    own_total = lax.dynamic_slice_in_dim(weight_total, head_start, head_count, 1)
    merged = merged_sum / own_total[:, :, None]
    projector = value_up.reshape(head_count, segment, VD).astype(jnp.float32)
    value_part = jnp.einsum("shl,hlv->shv", merged, projector, precision=lax.Precision.HIGHEST)
    holders = kv_count // H if kv_count > H else 1
    for bit in range(holders.bit_length() - 1):
        value_part = value_part + from_partner(value_part, "kv", bit)
    value_rows = value_part.astype(jnp.bfloat16).reshape(seq_count, head_count * VD)
    if holders > 1:
        value_rows = lax.dynamic_slice_in_dim(
            value_rows, shard_index % holders * out_rows, out_rows, 1
        )
    partial_out = jnp.dot(value_rows, out_proj, preferred_element_type=jnp.float32)
    experts_local = EXPERTS // kv_count
    slot_count = experts_local * CAP
    targets = slot_targets(expert_ids)
    own_match = slot_match(targets, shard_index * slot_count, slot_count)
    own_pick = token_picker(own_match, seq_count)
    slot_gate = jnp.dot(own_match, gate_weights.reshape(-1), precision=lax.Precision.HIGHEST)
    attn_rows = lax.psum(partial_out, "kv")
    resid_rows, gain_cols = (
        lax.all_gather(residual, "kv", axis=1, tiled=True),
        lax.all_gather(norm_gain, "kv", axis=0, tiled=True),
    )
    summed = attn_rows + resid_rows.astype(jnp.float32)
    inverse_rms = lax.rsqrt(jnp.mean(summed * summed, axis=1) + small_eps)
    normed = summed * inverse_rms[:, None] * gain_cols.astype(jnp.float32)
    peak_abs = jnp.max(jnp.abs(normed), axis=1) + small_eps
    coded_rows = (normed / peak_abs[:, None]).astype(jnp.bfloat16)
    dispatched = jnp.dot(
        own_pick.astype(jnp.bfloat16), coded_rows, preferred_element_type=jnp.float32
    ).astype(jnp.bfloat16)
    slot_scale = jnp.dot(own_pick, peak_abs, precision=lax.Precision.HIGHEST)
    return (
        dispatched.reshape(experts_local, CAP, D),
        slot_scale.reshape(experts_local, CAP),
        slot_gate.reshape(experts_local, CAP),
    )


CORES = 2
LINKED_Y = 2
LANES = 128
ROWS = 8
GROUP = 2
LAGS = (0, 2, 3, 5, 8, 11, 11, 13, 15, 18, 20, 22, 23)
F32 = jnp.float32
BF16 = jnp.bfloat16


def split3(value):
    first = value.astype(BF16).astype(F32)
    rest = value - first
    second = rest.astype(BF16).astype(F32)
    return first, second, rest - second


def put_lanes(shape, columns):
    lane = lax.broadcasted_iota(jnp.int32, shape, len(shape) - 1)
    tile = jnp.zeros(shape, F32)
    for index, column in columns:
        tile = jnp.where(lane == index, column, tile)
    return tile


def take3(tile, start):
    return (
        tile[..., start : start + 1]
        + tile[..., start + 1 : start + 2]
        + tile[..., start + 2 : start + 3]
    )


def merge(blocks):
    heads = (blocks[0].shape[-1] - LANES) // LAT
    outs, columns = [], []
    for head in range(heads):
        stats = [block[..., heads * LAT :] for block in blocks]
        maxes = [take3(stat, head * 6) for stat in stats]
        totals = [take3(stat, head * 6 + 3) for stat in stats]
        top = maxes[0]
        for other in maxes[1:]:
            top = jnp.maximum(top, other)
        total, out = 0.0, 0.0
        for block, own_max, own_total in zip(blocks, maxes, totals):
            factor = jnp.exp(own_max - top)
            total = total + factor * own_total
            out = out + factor * block[..., head * LAT : (head + 1) * LAT]
        outs.append((out, top, total))
    return outs


def message(outs):
    columns = []
    for head, (out, top, total) in enumerate(outs):
        for index, part in enumerate(split3(top) + split3(total)):
            columns.append((head * 6 + index, part))
    shape = outs[0][0].shape[:-1] + (LANES,)
    return jnp.concatenate([out for out, _, _ in outs] + [put_lanes(shape, columns)], axis=-1)


def step_kernel(
    zs,
    chunks,
    q_ref,
    cache_hbm,
    ctx_ref,
    up_ref,
    proj_hbm,
    resid_ref,
    gain_ref,
    ids_ref,
    gates_ref,
    out_ref,
    scale_ref,
    gate_ref,
    qown,
    pick_scr,
    cache,
    proj,
    qbuf,
    qrow,
    osc,
    msc,
    s1,
    r1,
    k1,
    r2,
    k2,
    r3,
    merged,
    mine,
    ps1,
    pr1,
    pk1,
    pr2,
    pk2,
    pr3,
    gbuf,
    codes,
    peaks,
    load_sem,
    proj_sem,
    qz_s,
    qz_r,
    q_s,
    q_r,
    oz_s,
    oz_r,
    o_s,
    o_r,
    pz_s,
    pz_r,
    p_s,
    p_r,
):
    me = lax.axis_index("kv")
    core = lax.rem(me, CORES)
    y = lax.rem(me // CORES, LINKED_Y)
    z = me // (CORES * LINKED_Y)

    def device(zz, yy, cc):
        return {"kv": (zz * LINKED_Y + yy) * CORES + cc}

    partner = device(z, y, 1 - core)
    across = device(z, 1 - y, core)
    along = [lax.rem(z + step, zs) for step in range(1, zs)]
    back = [lax.rem(z + zs - step, zs) for step in range(1, zs)]

    def copy(source, target, send, recv, where):
        return pltpu.make_async_remote_copy(
            src_ref=source,
            dst_ref=target,
            send_sem=send,
            recv_sem=recv,
            device_id=where,
            device_id_type=pl.DeviceIdType.MESH,
        )

    loads = [
        pltpu.make_async_copy(
            cache_hbm.at[pl.ds(k * ROWS, ROWS)], cache.at[pl.ds(k * ROWS, ROWS)], load_sem.at[k]
        )
        for k in range(chunks)
    ]
    for load in loads:
        load.start()
    proj_load = pltpu.make_async_copy(proj_hbm, proj, proj_sem)
    proj_load.start()

    raw = q_ref[...].astype(F32)
    key = LAT + ROPE
    qown[...] = jnp.concatenate(
        [raw[..., :LAT], raw[..., key : key + LAT], raw[..., LAT:key], raw[..., key + LAT :]],
        axis=-1,
    ).astype(BF16)

    ids, gates = ids_ref[...], gates_ref[...]
    experts, seqs = out_ref.shape[0], ids.shape[1]
    slots = experts * CAP
    earlier = lax.broadcasted_iota(jnp.int32, (seqs, seqs), 0) < lax.broadcasted_iota(
        jnp.int32, (seqs, seqs), 1
    )
    earlier = earlier.astype(F32).astype(BF16)
    line = lax.broadcasted_iota(jnp.int32, (slots, seqs), 0)

    def choose(expert, slot):
        member, gate = jnp.zeros((slots, seqs), F32), jnp.zeros((slots, seqs), F32)
        for choice in range(ids.shape[0]):
            same = ids[choice : choice + 1] == me * experts + expert
            member = jnp.where(same, 1.0, member)
            gate = jnp.where(same, gates[choice : choice + 1], gate)
        rank = jnp.dot(member.astype(BF16), earlier, preferred_element_type=F32)
        return jnp.where(jnp.abs(rank - slot.astype(F32)) < 0.5, member, 0.0), gate

    pick_scr[0] = choose(line // CAP, lax.rem(line, CAP))[0]
    by_slot, gate = choose(lax.rem(line, experts), line // experts)
    pick_scr[1] = by_slot
    slot_gates = jnp.sum(by_slot * gate, axis=1, keepdims=True)

    barrier = pltpu.get_barrier_semaphore()
    peers = [partner, across] + [device(zz, y, core) for zz in along]
    for peer in peers:
        pl.semaphore_signal(
            barrier, inc=1, device_id=peer, device_id_type=pl.DeviceIdType.MESH
        )
    pl.semaphore_wait(barrier, len(peers))

    pending = []

    def z_copies(source_of, target, send, recv):
        made = []
        for step, zz in enumerate(along):
            made.append(copy(source_of(zz), target, send.at[step], recv.at[step], device(zz, y, core)))
        return made

    def launch(made):
        for one in made:
            one.start()
            pending.append(one)
        return made

    q_along = [
        launch(z_copies(lambda zz: qown.at[k], qbuf.at[k, core, y, z], qz_s.at[k], qz_r.at[k]))
        for k in range(chunks)
    ]
    for k in range(chunks):
        qbuf[k, core, y, z] = qown[k]
    q_across, q_pair, o_pair, o_across, o_along = {}, {}, {}, {}, {}

    def gather_across(k):
        for one in q_along[k]:
            one.wait_recv()
        q_across[k] = launch(
            [copy(qbuf.at[k, core, y], qbuf.at[k, core, y], q_s.at[k, 0], q_r.at[k, 0], across)]
        )

    def gather_pair(k):
        q_across[k][0].wait_recv()
        q_pair[k] = launch(
            [copy(qbuf.at[k, core], qbuf.at[k, core], q_s.at[k, 1], q_r.at[k, 1], partner)]
        )

    ctx_local = cache.shape[2]
    count = CORES * LINKED_Y * zs
    position = me * ctx_local + lax.broadcasted_iota(jnp.int32, (2 * count, ctx_local), 1)

    def attend(k):
        q_pair[k][0].wait_recv()
        loads[k].wait()
        width = q_ref.shape[-1]
        rows = qbuf[k].reshape(count, ROWS, width).astype(F32)
        qrow[...] = jnp.swapaxes(rows, 0, 1).astype(BF16)

        scored = []
        for at in range(ROWS):
            row = qrow[at]
            latent = jnp.concatenate([row[:, :LAT], row[:, LAT : 2 * LAT]], axis=0)
            rotary = row[:, 2 * LAT :]
            rotary = jnp.concatenate([rotary[:, :ROPE], rotary[:, ROPE:]], axis=0)
            scores = jnp.dot(latent, cache[k * ROWS + at, :LAT], preferred_element_type=F32)
            scores = scores + jnp.dot(
                rotary, cache[k * ROWS + at, LAT:], preferred_element_type=F32
            )
            valid = position < ctx_ref[k * ROWS + at]
            scored.append(jnp.where(valid, scores * score_scale, masked_score))
        scores = jnp.stack(scored)
        top = jnp.max(scores, axis=2, keepdims=True)
        weights = jnp.where(scores > 0.5 * masked_score, jnp.exp(scores - top), 0.0)
        total = jnp.sum(weights, axis=2, keepdims=True)
        rounded = weights.astype(BF16)
        for at in range(ROWS):
            osc[at] = lax.dot_general(
                rounded[at],
                cache[k * ROWS + at, :LAT],
                (((1,), (1,)), ((), ())),
                preferred_element_type=F32,
            )
        columns = []
        for head in range(2):
            here = slice(head * count, (head + 1) * count)
            parts = split3(top[:, here]) + split3(total[:, here])
            columns += [(head * 6 + index, value) for index, value in enumerate(parts)]
        msc[...] = put_lanes((ROWS, count, LANES), columns)
        whole = jnp.swapaxes(osc[...], 0, 1).astype(BF16)
        shape = (CORES, LINKED_Y, zs, ROWS)
        s1[k, :, :, :, :, :LAT] = whole[:count].reshape(shape + (LAT,))
        s1[k, :, :, :, :, LAT : 2 * LAT] = whole[count:].reshape(shape + (LAT,))
        s1[k, :, :, :, :, 2 * LAT :] = (
            jnp.swapaxes(msc[...], 0, 1).astype(BF16).reshape(shape + (LANES,))
        )
        o_pair[k] = launch([copy(s1.at[k, 1 - core], r1.at[k], o_s.at[k, 0], o_r.at[k, 0], partner)])

    def merge_pair(k):
        o_pair[k][0].wait_recv()

        k1[k, 1 - y] = message(
            merge([s1[k, core, 1 - y].astype(F32), r1[k, 1 - y].astype(F32)])
        ).astype(BF16)
        o_across[k] = launch([copy(k1.at[k, 1 - y], r2.at[k], o_s.at[k, 1], o_r.at[k, 1], across)])

    def merge_across(k):
        o_across[k][0].wait_recv()

        k2[k] = message(
            merge([s1[k, core, y].astype(F32), r1[k, y].astype(F32), r2[k].astype(F32)])
        ).astype(BF16)
        o_along[k] = launch(
            [
                copy(k2.at[k, zz], r3.at[k, step], oz_s.at[k, step], oz_r.at[k, step], device(zz, y, core))
                for step, zz in enumerate(along)
            ]
        )

    def merge_along(k):
        for one in o_along[k]:
            one.wait_recv()
        blocks = [k2[k, z].astype(F32)] + [r3[k, step].astype(F32) for step in range(zs - 1)]
        for head, (out, _, total) in enumerate(merge(blocks)):
            merged[head, pl.ds(k * ROWS, ROWS), :] = out / total

    cols = resid_ref.shape[-1]
    chip_cols = cols * CORES
    p_pair, p_across, p_along, g_along, g_across, g_pair = {}, {}, {}, {}, {}, {}

    def span(g):
        first = g * GROUP
        return first, min(GROUP, chunks - first)

    def project(g):
        first, size = span(g)
        values = []
        for head in range(2):
            own = merged[head, pl.ds(first * ROWS, size * ROWS), :]
            high = own.astype(BF16)
            low = (own - high.astype(F32)).astype(BF16)
            rows = up_ref[head * LAT : (head + 1) * LAT]
            values.append(
                jnp.dot(high, rows, preferred_element_type=F32)
                + jnp.dot(low, rows, preferred_element_type=F32)
            )
        value = jnp.concatenate(values, axis=1).astype(BF16)
        if g == 0:
            proj_load.wait()
        here = pl.ds(first, size)
        for zz in range(zs):
            for yy in range(LINKED_Y):
                start = (zz * LINKED_Y + yy) * chip_cols
                both = jnp.dot(
                    value, proj[:, start : start + chip_cols], preferred_element_type=F32
                ).reshape(size, ROWS, chip_cols)
                low, high = both[..., :cols], both[..., cols:]
                mine[here, yy, zz] = jnp.where(core == 0, low, high)
                ps1[here, yy, zz] = jnp.where(core == 0, high, low).astype(BF16)
        p_pair[g] = launch([copy(ps1.at[here], pr1.at[here], p_s.at[g, 0], p_r.at[g, 0], partner)])

    def sum_pair(g):
        here = pl.ds(*span(g))
        p_pair[g][0].wait_recv()
        pk1[here] = (mine[here, 1 - y] + pr1[here, 1 - y].astype(F32)).astype(BF16)
        p_across[g] = launch([copy(pk1.at[here], pr2.at[here], p_s.at[g, 1], p_r.at[g, 1], across)])

    def sum_across(g):
        here = pl.ds(*span(g))
        p_across[g][0].wait_recv()
        kept = mine[here, y] + pr1[here, y].astype(F32) + pr2[here].astype(F32)
        mine[here, y] = kept
        pk2[here] = kept.astype(BF16)
        p_along[g] = launch(
            [
                copy(
                    pk2.at[here, zz],
                    pr3.at[step, here],
                    pz_s.at[g, 0, step],
                    pz_r.at[g, 0, step],
                    device(zz, y, core),
                )
                for step, zz in enumerate(along)
            ]
        )

    def sum_along(g):
        here = pl.ds(*span(g))
        for one in p_along[g]:
            one.wait_recv()
        summed = mine[here, y, z] + resid_ref[here].astype(F32)
        for step in range(zs - 1):
            summed = summed + pr3[step, here].astype(F32)
        scaled = summed * gain_ref[...].astype(F32)
        square = jnp.sum(summed * summed, axis=-1, keepdims=True)
        largest = jnp.max(jnp.abs(scaled), axis=-1, keepdims=True)
        shape = summed.shape[:-1] + (gbuf.shape[-1] - cols,)
        stats = put_lanes(shape, list(enumerate(split3(square) + split3(largest))))
        gbuf[here, core, y, z] = jnp.concatenate([scaled, stats], axis=-1).astype(BF16)
        block = gbuf.at[here, core, y, z]
        g_along[g] = launch(
            [
                copy(block, block, pz_s.at[g, 1, step], pz_r.at[g, 1, step], device(zz, y, core))
                for step, zz in enumerate(along)
            ]
        )

    def spread_across(g):
        here = pl.ds(*span(g))
        for one in g_along[g]:
            one.wait_recv()
        block = gbuf.at[here, core, y]
        g_across[g] = launch([copy(block, block, p_s.at[g, 2], p_r.at[g, 2], across)])

    def spread_pair(g):
        here = pl.ds(*span(g))
        g_across[g][0].wait_recv()
        block = gbuf.at[here, core]
        g_pair[g] = launch([copy(block, block, p_s.at[g, 3], p_r.at[g, 3], partner)])

    def finish(g):
        first, size = span(g)
        g_pair[g][0].wait_recv()
        for k in range(first, first + size):
            here = pl.ds(k * ROWS, ROWS)
            stats = gbuf[k, :, :, :, :, cols:].astype(F32).reshape(count, ROWS, -1)
            square = jnp.sum(take3(stats, 0), axis=0)
            largest = jnp.max(take3(stats, 3), axis=0)
            inverse = lax.rsqrt(square / (chip_cols * LINKED_Y * zs) + small_eps)
            peak = largest * inverse + small_eps
            factor = inverse / peak
            peaks[here] = jnp.broadcast_to(peak, (ROWS, LANES))
            for zz in range(zs):
                for yy in range(LINKED_Y):
                    start = (zz * LINKED_Y + yy) * chip_cols
                    rows = [gbuf[k, cc, yy, zz, :, :cols].astype(F32) for cc in range(CORES)]
                    codes[here, start : start + chip_cols] = (
                        jnp.concatenate(rows, axis=1) * factor
                    ).astype(BF16)

    chunk_stages = (gather_across, gather_pair, attend, merge_pair, merge_across, merge_along)
    group_stages = (
        project,
        sum_pair,
        sum_across,
        sum_along,
        spread_across,
        spread_pair,
        finish,
    )
    groups = -(-chunks // GROUP)
    order = []
    for rank, stage in enumerate(chunk_stages):
        for k in range(chunks):
            order.append((k + LAGS[rank], rank, stage, k))
    for rank, stage in enumerate(group_stages, len(chunk_stages)):
        for g in range(groups):
            order.append((sum(span(g)) - 1 + LAGS[rank], rank, stage, g))
    for _, _, stage, index in sorted(order, key=lambda entry: entry[:2]):
        stage(index)

    pick = pick_scr[0].astype(BF16)
    for start in range(0, codes.shape[1], chip_cols):
        out_ref[:, :, start : start + chip_cols] = (
            jnp.dot(pick, codes[:, start : start + chip_cols], preferred_element_type=F32)
            .reshape(experts, CAP, chip_cols)
            .astype(BF16)
        )
    scales = jnp.dot(
        pick_scr[1], peaks[...], precision=lax.Precision.HIGHEST, preferred_element_type=F32
    )
    wide = jnp.broadcast_to(slot_gates, (slots, LANES))
    tail = jnp.zeros((LANES - 2 * slots, LANES), F32)
    flat = jnp.transpose(jnp.concatenate([scales, wide, tail], axis=0))[:1]
    for slot in range(CAP):
        at = slot * experts
        scale_ref[slot : slot + 1] = flat[:, at : at + experts]
        gate_ref[slot : slot + 1] = flat[:, slots + at : slots + at + experts]
    for one in pending:
        one.wait_send()


def fused_device(
    queries,
    latent_cache,
    context_lengths,
    value_up,
    out_proj,
    residual,
    norm_gain,
    expert_ids,
    gate_weights,
):
    kv_count = lax.axis_size("kv")
    zs = kv_count // (CORES * LINKED_Y)
    seq_count = queries.shape[0]
    chunks = seq_count // ROWS
    ctx_local = latent_cache.shape[1]
    width = queries.shape[1]
    cols = residual.shape[1]
    chip_cols = cols * CORES
    held = -(-(cols + 6) // LANES) * LANES
    groups = -(-chunks // GROUP)
    experts_local = EXPERTS // kv_count
    slot_count = experts_local * CAP
    vmem = pl.BlockSpec(memory_space=pltpu.VMEM)
    smem = pl.BlockSpec(memory_space=pltpu.SMEM)
    anywhere = pl.BlockSpec(memory_space=pl.ANY)
    dma = pltpu.SemaphoreType.DMA
    full = (LINKED_Y, zs)
    dispatched, scale, gate = pl.pallas_call(
        functools.partial(step_kernel, zs, chunks),
        out_shape=(
            jax.ShapeDtypeStruct((experts_local, CAP, chip_cols * LINKED_Y * zs), BF16),
            jax.ShapeDtypeStruct((CAP, experts_local), F32),
            jax.ShapeDtypeStruct((CAP, experts_local), F32),
        ),
        in_specs=[vmem, anywhere, smem, vmem, anywhere, vmem, vmem, vmem, vmem],
        out_specs=(vmem, vmem, vmem),
        scratch_shapes=[
            pltpu.VMEM((chunks, ROWS, width), BF16),
            pltpu.VMEM((2, slot_count, seq_count), F32),
            pltpu.VMEM((seq_count, LAT + ROPE, ctx_local), BF16),
            pltpu.VMEM(out_proj.shape, BF16),
            pltpu.VMEM((chunks, CORES) + full + (ROWS, width), BF16),
            pltpu.VMEM((ROWS, kv_count, width), BF16),
            pltpu.VMEM((ROWS, H, LAT), F32),
            pltpu.VMEM((ROWS, kv_count, LANES), F32),
            pltpu.VMEM((chunks, CORES) + full + (ROWS, width), BF16),
            pltpu.VMEM((chunks,) + full + (ROWS, width), BF16),
            pltpu.VMEM((chunks,) + full + (ROWS, width), BF16),
            pltpu.VMEM((chunks, zs, ROWS, width), BF16),
            pltpu.VMEM((chunks, zs, ROWS, width), BF16),
            pltpu.VMEM((chunks, zs - 1, ROWS, width), BF16),
            pltpu.VMEM((H // kv_count, seq_count, LAT), F32),
            pltpu.VMEM((chunks,) + full + (ROWS, cols), F32),
            pltpu.VMEM((chunks,) + full + (ROWS, cols), BF16),
            pltpu.VMEM((chunks,) + full + (ROWS, cols), BF16),
            pltpu.VMEM((chunks, zs, ROWS, cols), BF16),
            pltpu.VMEM((chunks, zs, ROWS, cols), BF16),
            pltpu.VMEM((chunks, zs, ROWS, cols), BF16),
            pltpu.VMEM((zs - 1, chunks, ROWS, cols), BF16),
            pltpu.VMEM((chunks, CORES) + full + (ROWS, held), BF16),
            pltpu.VMEM((seq_count, chip_cols * LINKED_Y * zs), BF16),
            pltpu.VMEM((seq_count, LANES), F32),
            dma((chunks,)),
            dma,
            dma((chunks, zs - 1)),
            dma((chunks, zs - 1)),
            dma((chunks, 2)),
            dma((chunks, 2)),
            dma((chunks, zs - 1)),
            dma((chunks, zs - 1)),
            dma((chunks, 2)),
            dma((chunks, 2)),
            dma((groups, 2, zs - 1)),
            dma((groups, 2, zs - 1)),
            dma((groups, 4)),
            dma((groups, 4)),
        ],
        compiler_params=pltpu.CompilerParams(
            collective_id=0, has_side_effects=True, vmem_limit_bytes=60 * 1024 * 1024
        ),
    )(
        queries.reshape(chunks, ROWS, width),
        jnp.swapaxes(latent_cache, 1, 2),
        context_lengths,
        value_up,
        out_proj,
        residual.reshape(chunks, ROWS, cols),
        norm_gain.reshape(1, -1),
        expert_ids.T,
        gate_weights.T,
    )
    return dispatched, scale.T, gate.T


def per_device(*arrays):
    queries, residual = arrays[0], arrays[5]
    kv_count = lax.axis_size("kv")
    pairs = H == 2 * kv_count and EXPERTS * CAP * 2 <= kv_count * LANES and 2 * ROPE == LANES and kv_count % (CORES * LINKED_Y) == 0
    aligned = queries.shape[0] % ROWS == 0 and residual.shape[1] * CORES % LANES == 0
    if pairs and aligned:
        return fused_device(*arrays)
    return general_device(*arrays)


def solution(mesh):
    in_specs = (
        P("groups", "kv"),
        P("groups", "kv", None),
        P("groups"),
        P("kv", None),
        P("kv", None),
        P("groups", "kv"),
        P("kv"),
        P("groups", None),
        P("groups", None),
    )
    out_specs = (
        P(("groups", "kv"), None, None),
        P(("groups", "kv"), None),
        P(("groups", "kv"), None),
    )
    return jax.shard_map(
        per_device, mesh=mesh, in_specs=in_specs, out_specs=out_specs, check_vma=False
    )
```

```python
import functools

import jax
import jax.numpy as jnp
from jax import lax
from jax.experimental import pallas as pl
from jax.experimental.pallas import tpu as pltpu
from jax.sharding import PartitionSpec as P

H = 32
LAT = 512
ROPE = 64
VD = 128
D = 7168
EXPERTS = 256
TOPK = 8
CAP = 2


score_scale = 192.0 ** (-0.5)
masked_score = -1e30
small_eps = 1e-06


def from_partner(value, axis, bit):
    mask = 2**bit
    pairs = [(source, source ^ mask) for source in range(lax.axis_size(axis))]
    return lax.ppermute(value, axis, pairs)


def slot_targets(expert_ids):
    flat_ids = expert_ids.reshape(-1)
    order_index = jnp.arange(flat_ids.shape[0], dtype=jnp.int32)
    same_before = (flat_ids[:, None] == flat_ids[None, :]) & (
        order_index[None, :] < order_index[:, None]
    )
    rank_within = jnp.sum(same_before.astype(jnp.int32), axis=1)
    return flat_ids * CAP + rank_within


def slot_match(targets, first_slot, slot_count):
    slot_index = first_slot + jnp.arange(slot_count, dtype=jnp.int32)
    return (slot_index[:, None] == targets[None, :]).astype(jnp.float32)


def token_picker(matches, seq_count):
    return jnp.sum(matches.reshape(matches.shape[0], seq_count, TOPK), axis=2)


def general_device(
    queries,
    latent_cache,
    context_lengths,
    value_up,
    out_proj,
    residual,
    norm_gain,
    expert_ids,
    gate_weights,
):
    kv_count = lax.axis_size("kv")
    shard_index = lax.axis_index("kv")
    seq_count = queries.shape[0]
    query_rows = lax.all_gather(queries, "kv", axis=1, tiled=True).reshape(seq_count, H, LAT + ROPE)
    ctx_local = latent_cache.shape[1]
    scores = (
        jnp.einsum("shq,scq->shc", query_rows, latent_cache, preferred_element_type=jnp.float32)
        * score_scale
    )
    position = shard_index * ctx_local + jnp.arange(ctx_local, dtype=jnp.int32)
    valid_mask = (position[None, :] < context_lengths[:, None])[:, None, :]
    scores = jnp.where(valid_mask, scores, masked_score)
    local_max = jnp.max(scores, axis=2)
    weights = jnp.where(valid_mask, jnp.exp(scores - local_max[:, :, None]), 0.0)
    local_total = jnp.sum(weights, axis=2)
    local_out = jnp.einsum(
        "shc,scl->shl",
        weights.astype(jnp.bfloat16),
        latent_cache[:, :, :LAT],
        preferred_element_type=jnp.float32,
    )
    out_rows = out_proj.shape[0]
    col_count = H * LAT // kv_count
    segment = min(col_count, LAT)
    head_count = col_count // segment
    head_start = shard_index * col_count // LAT
    global_max = lax.pmax(local_max, "kv")
    scaling = jnp.exp(local_max - global_max)
    weight_total = lax.psum(local_total * scaling, "kv")
    scaled = (local_out * scaling[:, :, None]).reshape(seq_count, H * LAT)
    merged_sum = lax.psum_scatter(scaled, "kv", scatter_dimension=1, tiled=True).reshape(
        seq_count, head_count, segment
    )
    own_total = lax.dynamic_slice_in_dim(weight_total, head_start, head_count, 1)
    merged = merged_sum / own_total[:, :, None]
    projector = value_up.reshape(head_count, segment, VD).astype(jnp.float32)
    value_part = jnp.einsum("shl,hlv->shv", merged, projector, precision=lax.Precision.HIGHEST)
    holders = kv_count // H if kv_count > H else 1
    for bit in range(holders.bit_length() - 1):
        value_part = value_part + from_partner(value_part, "kv", bit)
    value_rows = value_part.astype(jnp.bfloat16).reshape(seq_count, head_count * VD)
    if holders > 1:
        value_rows = lax.dynamic_slice_in_dim(
            value_rows, shard_index % holders * out_rows, out_rows, 1
        )
    partial_out = jnp.dot(value_rows, out_proj, preferred_element_type=jnp.float32)
    experts_local = EXPERTS // kv_count
    slot_count = experts_local * CAP
    targets = slot_targets(expert_ids)
    own_match = slot_match(targets, shard_index * slot_count, slot_count)
    own_pick = token_picker(own_match, seq_count)
    slot_gate = jnp.dot(own_match, gate_weights.reshape(-1), precision=lax.Precision.HIGHEST)
    attn_rows = lax.psum(partial_out, "kv")
    resid_rows, gain_cols = (
        lax.all_gather(residual, "kv", axis=1, tiled=True),
        lax.all_gather(norm_gain, "kv", axis=0, tiled=True),
    )
    summed = attn_rows + resid_rows.astype(jnp.float32)
    inverse_rms = lax.rsqrt(jnp.mean(summed * summed, axis=1) + small_eps)
    normed = summed * inverse_rms[:, None] * gain_cols.astype(jnp.float32)
    peak_abs = jnp.max(jnp.abs(normed), axis=1) + small_eps
    coded_rows = (normed / peak_abs[:, None]).astype(jnp.bfloat16)
    dispatched = jnp.dot(
        own_pick.astype(jnp.bfloat16), coded_rows, preferred_element_type=jnp.float32
    ).astype(jnp.bfloat16)
    slot_scale = jnp.dot(own_pick, peak_abs, precision=lax.Precision.HIGHEST)
    return (
        dispatched.reshape(experts_local, CAP, D),
        slot_scale.reshape(experts_local, CAP),
        slot_gate.reshape(experts_local, CAP),
    )


CORES = 2
LINKED_Y = 2
LANES = 128
ROWS = 8
GROUP = 1
LAGS = (0, 2, 3, 4.5, 8, 12, 12, 13, 15, 18, 20, 22, 23)
F32 = jnp.float32
BF16 = jnp.bfloat16


def split3(value):
    first = value.astype(BF16).astype(F32)
    rest = value - first
    second = rest.astype(BF16).astype(F32)
    return first, second, rest - second


def put_lanes(shape, columns):
    lane = lax.broadcasted_iota(jnp.int32, shape, len(shape) - 1)
    tile = jnp.zeros(shape, F32)
    for index, column in columns:
        tile = jnp.where(lane == index, column, tile)
    return tile


def take3(tile, start):
    return (
        tile[..., start : start + 1]
        + tile[..., start + 1 : start + 2]
        + tile[..., start + 2 : start + 3]
    )


def merge(blocks):
    heads = (blocks[0].shape[-1] - LANES) // LAT
    outs, columns = [], []
    for head in range(heads):
        stats = [block[..., heads * LAT :] for block in blocks]
        maxes = [take3(stat, head * 6) for stat in stats]
        totals = [take3(stat, head * 6 + 3) for stat in stats]
        top = maxes[0]
        for other in maxes[1:]:
            top = jnp.maximum(top, other)
        total, out = 0.0, 0.0
        for block, own_max, own_total in zip(blocks, maxes, totals):
            factor = jnp.exp(own_max - top)
            total = total + factor * own_total
            out = out + factor * block[..., head * LAT : (head + 1) * LAT]
        outs.append((out, top, total))
    return outs


def message(outs):
    columns = []
    for head, (out, top, total) in enumerate(outs):
        for index, part in enumerate(split3(top) + split3(total)):
            columns.append((head * 6 + index, part))
    shape = outs[0][0].shape[:-1] + (LANES,)
    return jnp.concatenate([out for out, _, _ in outs] + [put_lanes(shape, columns)], axis=-1)


def step_kernel(
    zs,
    chunks,
    q_ref,
    cache_hbm,
    ctx_ref,
    up_ref,
    proj_hbm,
    resid_ref,
    gain_ref,
    codes,
    peaks,
    qown,
    cache,
    proj,
    qbuf,
    qrow,
    osc,
    msc,
    s1,
    r1,
    k1,
    r2,
    k2,
    r3,
    merged,
    mine,
    ps1,
    pr1,
    pk1,
    pr2,
    pk2,
    pr3,
    gbuf,
    load_sem,
    proj_sem,
    qz_s,
    qz_r,
    q_s,
    q_r,
    oz_s,
    oz_r,
    o_s,
    o_r,
    pz_s,
    pz_r,
    p_s,
    p_r,
):
    me = lax.axis_index("kv")
    core = lax.rem(me, CORES)
    y = lax.rem(me // CORES, LINKED_Y)
    z = me // (CORES * LINKED_Y)

    def device(zz, yy, cc):
        return {"kv": (zz * LINKED_Y + yy) * CORES + cc}

    partner = device(z, y, 1 - core)
    across = device(z, 1 - y, core)
    along = [lax.rem(z + step, zs) for step in range(1, zs)]
    back = [lax.rem(z + zs - step, zs) for step in range(1, zs)]

    def copy(source, target, send, recv, where):
        return pltpu.make_async_remote_copy(
            src_ref=source,
            dst_ref=target,
            send_sem=send,
            recv_sem=recv,
            device_id=where,
            device_id_type=pl.DeviceIdType.MESH,
        )

    loads = [
        pltpu.make_async_copy(
            cache_hbm.at[pl.ds(k * ROWS, ROWS)], cache.at[pl.ds(k * ROWS, ROWS)], load_sem.at[k]
        )
        for k in range(chunks)
    ]
    for load in loads:
        load.start()
    proj_load = pltpu.make_async_copy(proj_hbm, proj, proj_sem)
    proj_load.start()

    raw = q_ref[...].astype(F32)
    key = LAT + ROPE
    qown[...] = jnp.concatenate(
        [raw[..., :LAT], raw[..., key : key + LAT], raw[..., LAT:key], raw[..., key + LAT :]],
        axis=-1,
    ).astype(BF16)

    barrier = pltpu.get_barrier_semaphore()
    peers = [partner, across] + [device(zz, y, core) for zz in along]
    for peer in peers:
        pl.semaphore_signal(
            barrier, inc=1, device_id=peer, device_id_type=pl.DeviceIdType.MESH
        )
    pl.semaphore_wait(barrier, len(peers))

    pending = []

    def z_copies(source_of, target, send, recv):
        made = []
        for step, zz in enumerate(along):
            made.append(copy(source_of(zz), target, send.at[step], recv.at[step], device(zz, y, core)))
        return made

    def launch(made):
        for one in made:
            one.start()
            pending.append(one)
        return made

    q_along = [
        launch(z_copies(lambda zz: qown.at[k], qbuf.at[k, core, y, z], qz_s.at[k], qz_r.at[k]))
        for k in range(chunks)
    ]
    for k in range(chunks):
        qbuf[k, core, y, z] = qown[k]
    q_across, q_pair, o_pair, o_across, o_along = {}, {}, {}, {}, {}

    def gather_across(k):
        for one in q_along[k]:
            one.wait_recv()
        q_across[k] = launch(
            [copy(qbuf.at[k, core, y], qbuf.at[k, core, y], q_s.at[k, 0], q_r.at[k, 0], across)]
        )

    def gather_pair(k):
        q_across[k][0].wait_recv()
        q_pair[k] = launch(
            [copy(qbuf.at[k, core], qbuf.at[k, core], q_s.at[k, 1], q_r.at[k, 1], partner)]
        )

    ctx_local = cache.shape[2]
    count = CORES * LINKED_Y * zs
    position = me * ctx_local + lax.broadcasted_iota(jnp.int32, (2 * count, ctx_local), 1)

    def attend(k):
        q_pair[k][0].wait_recv()
        loads[k].wait()
        width = q_ref.shape[-1]
        rows = qbuf[k].reshape(count, ROWS, width).astype(F32)
        qrow[...] = jnp.swapaxes(rows, 0, 1).astype(BF16)

        scored = []
        for at in range(ROWS):
            row = qrow[at]
            latent = jnp.concatenate([row[:, :LAT], row[:, LAT : 2 * LAT]], axis=0)
            rotary = row[:, 2 * LAT :]
            rotary = jnp.concatenate([rotary[:, :ROPE], rotary[:, ROPE:]], axis=0)
            scores = jnp.dot(latent, cache[k * ROWS + at, :LAT], preferred_element_type=F32)
            scores = scores + jnp.dot(
                rotary, cache[k * ROWS + at, LAT:], preferred_element_type=F32
            )
            valid = position < ctx_ref[k * ROWS + at]
            scored.append(jnp.where(valid, scores * score_scale, masked_score))
        scores = jnp.stack(scored)
        top = jnp.max(scores, axis=2, keepdims=True)
        weights = jnp.where(scores > 0.5 * masked_score, jnp.exp(scores - top), 0.0)
        total = jnp.sum(weights, axis=2, keepdims=True)
        rounded = weights.astype(BF16)
        for at in range(ROWS):
            osc[at] = lax.dot_general(
                rounded[at],
                cache[k * ROWS + at, :LAT],
                (((1,), (1,)), ((), ())),
                preferred_element_type=F32,
            )
        columns = []
        for head in range(2):
            here = slice(head * count, (head + 1) * count)
            parts = split3(top[:, here]) + split3(total[:, here])
            columns += [(head * 6 + index, value) for index, value in enumerate(parts)]
        msc[...] = put_lanes((ROWS, count, LANES), columns)
        whole = jnp.swapaxes(osc[...], 0, 1).astype(BF16)
        shape = (CORES, LINKED_Y, zs, ROWS)
        s1[k, :, :, :, :, :LAT] = whole[:count].reshape(shape + (LAT,))
        s1[k, :, :, :, :, LAT : 2 * LAT] = whole[count:].reshape(shape + (LAT,))
        s1[k, :, :, :, :, 2 * LAT :] = (
            jnp.swapaxes(msc[...], 0, 1).astype(BF16).reshape(shape + (LANES,))
        )
        o_pair[k] = launch([copy(s1.at[k, 1 - core], r1.at[k], o_s.at[k, 0], o_r.at[k, 0], partner)])

    def merge_pair(k):
        o_pair[k][0].wait_recv()

        k1[k, 1 - y] = message(
            merge([s1[k, core, 1 - y].astype(F32), r1[k, 1 - y].astype(F32)])
        ).astype(BF16)
        o_across[k] = launch([copy(k1.at[k, 1 - y], r2.at[k], o_s.at[k, 1], o_r.at[k, 1], across)])

    def merge_across(k):
        o_across[k][0].wait_recv()

        k2[k] = message(
            merge([s1[k, core, y].astype(F32), r1[k, y].astype(F32), r2[k].astype(F32)])
        ).astype(BF16)
        o_along[k] = launch(
            [
                copy(k2.at[k, zz], r3.at[k, step], oz_s.at[k, step], oz_r.at[k, step], device(zz, y, core))
                for step, zz in enumerate(along)
            ]
        )

    def merge_along(k):
        for one in o_along[k]:
            one.wait_recv()
        blocks = [k2[k, z].astype(F32)] + [r3[k, step].astype(F32) for step in range(zs - 1)]
        for head, (out, _, total) in enumerate(merge(blocks)):
            merged[head, pl.ds(k * ROWS, ROWS), :] = out / total

    cols = resid_ref.shape[-1]
    chip_cols = cols * CORES
    p_pair, p_across, p_along, g_along, g_across, g_pair = {}, {}, {}, {}, {}, {}

    def span(g):
        first = g * GROUP
        return first, min(GROUP, chunks - first)

    def project(g):
        first, size = span(g)
        values = []
        for head in range(2):
            own = merged[head, pl.ds(first * ROWS, size * ROWS), :]
            high = own.astype(BF16)
            low = (own - high.astype(F32)).astype(BF16)
            rows = up_ref[head * LAT : (head + 1) * LAT]
            values.append(
                jnp.dot(high, rows, preferred_element_type=F32)
                + jnp.dot(low, rows, preferred_element_type=F32)
            )
        value = jnp.concatenate(values, axis=1).astype(BF16)
        if g == 0:
            proj_load.wait()
        here = pl.ds(first, size)
        for zz in range(zs):
            for yy in range(LINKED_Y):
                start = (zz * LINKED_Y + yy) * chip_cols
                both = jnp.dot(
                    value, proj[:, start : start + chip_cols], preferred_element_type=F32
                ).reshape(size, ROWS, chip_cols)
                low, high = both[..., :cols], both[..., cols:]
                mine[here, yy, zz] = jnp.where(core == 0, low, high)
                ps1[here, yy, zz] = jnp.where(core == 0, high, low).astype(BF16)
        p_pair[g] = launch([copy(ps1.at[here], pr1.at[here], p_s.at[g, 0], p_r.at[g, 0], partner)])

    def sum_pair(g):
        here = pl.ds(*span(g))
        p_pair[g][0].wait_recv()
        pk1[here] = (mine[here, 1 - y] + pr1[here, 1 - y].astype(F32)).astype(BF16)
        p_across[g] = launch([copy(pk1.at[here], pr2.at[here], p_s.at[g, 1], p_r.at[g, 1], across)])

    def sum_across(g):
        here = pl.ds(*span(g))
        p_across[g][0].wait_recv()
        kept = mine[here, y] + pr1[here, y].astype(F32) + pr2[here].astype(F32)
        mine[here, y] = kept
        pk2[here] = kept.astype(BF16)
        p_along[g] = launch(
            [
                copy(
                    pk2.at[here, zz],
                    pr3.at[step, here],
                    pz_s.at[g, 0, step],
                    pz_r.at[g, 0, step],
                    device(zz, y, core),
                )
                for step, zz in enumerate(along)
            ]
        )

    def sum_along(g):
        here = pl.ds(*span(g))
        for one in p_along[g]:
            one.wait_recv()
        summed = mine[here, y, z] + resid_ref[here].astype(F32)
        for step in range(zs - 1):
            summed = summed + pr3[step, here].astype(F32)
        scaled = summed * gain_ref[...].astype(F32)
        square = jnp.sum(summed * summed, axis=-1, keepdims=True)
        largest = jnp.max(jnp.abs(scaled), axis=-1, keepdims=True)
        shape = summed.shape[:-1] + (gbuf.shape[-1] - cols,)
        stats = put_lanes(shape, list(enumerate(split3(square) + split3(largest))))
        gbuf[here, core, y, z] = jnp.concatenate([scaled, stats], axis=-1).astype(BF16)
        block = gbuf.at[here, core, y, z]
        g_along[g] = launch(
            [
                copy(block, block, pz_s.at[g, 1, step], pz_r.at[g, 1, step], device(zz, y, core))
                for step, zz in enumerate(along)
            ]
        )

    def spread_across(g):
        here = pl.ds(*span(g))
        for one in g_along[g]:
            one.wait_recv()
        block = gbuf.at[here, core, y]
        g_across[g] = launch([copy(block, block, p_s.at[g, 2], p_r.at[g, 2], across)])

    def spread_pair(g):
        here = pl.ds(*span(g))
        g_across[g][0].wait_recv()
        block = gbuf.at[here, core]
        g_pair[g] = launch([copy(block, block, p_s.at[g, 3], p_r.at[g, 3], partner)])

    def finish(g):
        first, size = span(g)
        g_pair[g][0].wait_recv()
        for k in range(first, first + size):
            here = pl.ds(k * ROWS, ROWS)
            stats = gbuf[k, :, :, :, :, cols:].astype(F32).reshape(count, ROWS, -1)
            square = jnp.sum(take3(stats, 0), axis=0)
            largest = jnp.max(take3(stats, 3), axis=0)
            inverse = lax.rsqrt(square / (chip_cols * LINKED_Y * zs) + small_eps)
            peak = largest * inverse + small_eps
            factor = inverse / peak
            peaks[here] = jnp.broadcast_to(peak, (ROWS, LANES))
            for zz in range(zs):
                for yy in range(LINKED_Y):
                    start = (zz * LINKED_Y + yy) * chip_cols
                    rows = [gbuf[k, cc, yy, zz, :, :cols].astype(F32) for cc in range(CORES)]
                    codes[here, start : start + chip_cols] = (
                        jnp.concatenate(rows, axis=1) * factor
                    ).astype(BF16)

    chunk_stages = (gather_across, gather_pair, attend, merge_pair, merge_across, merge_along)
    group_stages = (
        project,
        sum_pair,
        sum_across,
        sum_along,
        spread_across,
        spread_pair,
        finish,
    )
    groups = -(-chunks // GROUP)
    order = []
    for rank, stage in enumerate(chunk_stages):
        for k in range(chunks):
            order.append((k + LAGS[rank], rank, stage, k))
    for rank, stage in enumerate(group_stages, len(chunk_stages)):
        for g in range(groups):
            order.append((sum(span(g)) - 1 + LAGS[rank], rank, stage, g))
    for _, _, stage, index in sorted(order, key=lambda entry: entry[:2]):
        stage(index)

    for one in pending:
        one.wait_send()


def dispatch_kernel(width, codes, peaks, ids_ref, gates_ref, out_ref, scale_ref, gate_ref):
    me = lax.axis_index("kv")
    ids, gates = ids_ref[...], gates_ref[...]
    experts, seqs = out_ref.shape[0], ids.shape[1]
    slots = experts * CAP
    earlier = lax.broadcasted_iota(jnp.int32, (seqs, seqs), 0) < lax.broadcasted_iota(
        jnp.int32, (seqs, seqs), 1
    )
    earlier = earlier.astype(F32).astype(BF16)
    line = lax.broadcasted_iota(jnp.int32, (slots, seqs), 0)

    def choose(expert, slot):
        member, gate = jnp.zeros((slots, seqs), F32), jnp.zeros((slots, seqs), F32)
        for choice in range(ids.shape[0]):
            same = ids[choice : choice + 1] == me * experts + expert
            member = jnp.where(same, 1.0, member)
            gate = jnp.where(same, gates[choice : choice + 1], gate)
        rank = jnp.dot(member.astype(BF16), earlier, preferred_element_type=F32)
        return jnp.where(jnp.abs(rank - slot.astype(F32)) < 0.5, member, 0.0), gate

    pick = choose(line // CAP, lax.rem(line, CAP))[0].astype(BF16)
    by_slot, gate = choose(lax.rem(line, experts), line // experts)
    slot_gates = jnp.sum(by_slot * gate, axis=1, keepdims=True)

    for start in range(0, codes.shape[1], width):
        out_ref[:, :, start : start + width] = (
            jnp.dot(pick, codes[:, start : start + width], preferred_element_type=F32)
            .reshape(experts, CAP, width)
            .astype(BF16)
        )
    scales = jnp.dot(
        by_slot, peaks[...], precision=lax.Precision.HIGHEST, preferred_element_type=F32
    )
    wide = jnp.broadcast_to(slot_gates, (slots, LANES))
    tail = jnp.zeros((LANES - 2 * slots, LANES), F32)
    flat = jnp.transpose(jnp.concatenate([scales, wide, tail], axis=0))[:1]
    for slot in range(CAP):
        at = slot * experts
        scale_ref[slot : slot + 1] = flat[:, at : at + experts]
        gate_ref[slot : slot + 1] = flat[:, slots + at : slots + at + experts]


def fused_device(
    queries,
    latent_cache,
    context_lengths,
    value_up,
    out_proj,
    residual,
    norm_gain,
    expert_ids,
    gate_weights,
):
    kv_count = lax.axis_size("kv")
    zs = kv_count // (CORES * LINKED_Y)
    seq_count = queries.shape[0]
    chunks = seq_count // ROWS
    ctx_local = latent_cache.shape[1]
    width = queries.shape[1]
    cols = residual.shape[1]
    chip_cols = cols * CORES
    held = -(-(cols + 6) // LANES) * LANES
    groups = -(-chunks // GROUP)
    experts_local = EXPERTS // kv_count
    vmem = pl.BlockSpec(memory_space=pltpu.VMEM)
    smem = pl.BlockSpec(memory_space=pltpu.SMEM)
    anywhere = pl.BlockSpec(memory_space=pl.ANY)
    dma = pltpu.SemaphoreType.DMA
    full = (LINKED_Y, zs)
    codes, peaks = pl.pallas_call(
        functools.partial(step_kernel, zs, chunks),
        out_shape=(
            jax.ShapeDtypeStruct((seq_count, chip_cols * LINKED_Y * zs), BF16),
            jax.ShapeDtypeStruct((seq_count, LANES), F32),
        ),
        in_specs=[vmem, anywhere, smem, vmem, anywhere, vmem, vmem],
        out_specs=(vmem, vmem),
        scratch_shapes=[
            pltpu.VMEM((chunks, ROWS, width), BF16),
            pltpu.VMEM((seq_count, LAT + ROPE, ctx_local), BF16),
            pltpu.VMEM(out_proj.shape, BF16),
            pltpu.VMEM((chunks, CORES) + full + (ROWS, width), BF16),
            pltpu.VMEM((ROWS, kv_count, width), BF16),
            pltpu.VMEM((ROWS, H, LAT), F32),
            pltpu.VMEM((ROWS, kv_count, LANES), F32),
            pltpu.VMEM((chunks, CORES) + full + (ROWS, width), BF16),
            pltpu.VMEM((chunks,) + full + (ROWS, width), BF16),
            pltpu.VMEM((chunks,) + full + (ROWS, width), BF16),
            pltpu.VMEM((chunks, zs, ROWS, width), BF16),
            pltpu.VMEM((chunks, zs, ROWS, width), BF16),
            pltpu.VMEM((chunks, zs - 1, ROWS, width), BF16),
            pltpu.VMEM((H // kv_count, seq_count, LAT), F32),
            pltpu.VMEM((chunks,) + full + (ROWS, cols), F32),
            pltpu.VMEM((chunks,) + full + (ROWS, cols), BF16),
            pltpu.VMEM((chunks,) + full + (ROWS, cols), BF16),
            pltpu.VMEM((chunks, zs, ROWS, cols), BF16),
            pltpu.VMEM((chunks, zs, ROWS, cols), BF16),
            pltpu.VMEM((chunks, zs, ROWS, cols), BF16),
            pltpu.VMEM((zs - 1, chunks, ROWS, cols), BF16),
            pltpu.VMEM((chunks, CORES) + full + (ROWS, held), BF16),
            dma((chunks,)),
            dma,
            dma((chunks, zs - 1)),
            dma((chunks, zs - 1)),
            dma((chunks, 2)),
            dma((chunks, 2)),
            dma((chunks, zs - 1)),
            dma((chunks, zs - 1)),
            dma((chunks, 2)),
            dma((chunks, 2)),
            dma((groups, 2, zs - 1)),
            dma((groups, 2, zs - 1)),
            dma((groups, 4)),
            dma((groups, 4)),
        ],
        compiler_params=pltpu.CompilerParams(
            collective_id=0, has_side_effects=True, vmem_limit_bytes=60 * 1024 * 1024
        ),
    )(
        queries.reshape(chunks, ROWS, width),
        jnp.swapaxes(latent_cache, 1, 2),
        context_lengths,
        value_up,
        out_proj,
        residual.reshape(chunks, ROWS, cols),
        norm_gain.reshape(1, -1),
    )
    dispatched, scale, gate = pl.pallas_call(
        functools.partial(dispatch_kernel, chip_cols),
        out_shape=(
            jax.ShapeDtypeStruct((experts_local, CAP, codes.shape[1]), BF16),
            jax.ShapeDtypeStruct((CAP, experts_local), F32),
            jax.ShapeDtypeStruct((CAP, experts_local), F32),
        ),
        in_specs=[vmem] * 4,
        out_specs=(vmem, vmem, vmem),
    )(codes, peaks, expert_ids.T, gate_weights.T)
    return dispatched, scale.T, gate.T


def per_device(*arrays):
    queries, residual = arrays[0], arrays[5]
    kv_count = lax.axis_size("kv")
    pairs = H == 2 * kv_count and EXPERTS * CAP * 2 <= kv_count * LANES and 2 * ROPE == LANES and kv_count % (CORES * LINKED_Y) == 0
    aligned = queries.shape[0] % ROWS == 0 and residual.shape[1] * CORES % LANES == 0
    if pairs and aligned:
        return fused_device(*arrays)
    return general_device(*arrays)


def solution(mesh):
    in_specs = (
        P("groups", "kv"),
        P("groups", "kv", None),
        P("groups"),
        P("kv", None),
        P("kv", None),
        P("groups", "kv"),
        P("kv"),
        P("groups", None),
        P("groups", None),
    )
    out_specs = (
        P(("groups", "kv"), None, None),
        P(("groups", "kv"), None),
        P(("groups", "kv"), None),
    )
    return jax.shard_map(
        per_device, mesh=mesh, in_specs=in_specs, out_specs=out_specs, check_vma=False
    )
```
